32 devices in a mesh: shard: 8 (over z, y), width: 4 (over x, core).
Axes of the slice: x: 2, y: 2, z: 4, core: 2. Of those that a mesh axis runs over, the one named last changes fastest.
Arguments:
- weight_gate: float32 [2048, 8192], P('shard', 'width'), may hold values from -0.1875 to 0.1875
- moment_gate: float32 [2048, 8192], P('shard', 'width'), may hold values from -6 to 6
- square_gate: float32 [2048, 8192], P('shard', 'width'), may hold values from 0.1 to 10
- weight_up: float32 [2048, 8192], P('shard', 'width'), may hold values from -0.1875 to 0.1875
- moment_up: float32 [2048, 8192], P('shard', 'width'), may hold values from -6 to 6
- square_up: float32 [2048, 8192], P('shard', 'width'), may hold values from 0.1 to 10
- norm_train: float32 [2048], P(('shard', 'width')), may hold values from 0.25 to 1.75
- norm_step: float32 [2048], P(('shard', 'width')), may hold values from -0.3 to 0.3
Outputs:
- serving_gate: bfloat16 [2048, 8192], P(None, 'width')
- serving_up: bfloat16 [2048, 8192], P(None, 'width')
- scale_gate: float32 [8192], P('width')
- scale_up: float32 [8192], P('width')
- serve_norm: bfloat16 [2048], replicated
- whole_gate: float32 [2048, 8192], P('shard', 'width')
- whole_up: float32 [2048, 8192], P('shard', 'width')
The draws below stay inside these ranges and needn't reach their ends.
All inputs are finite; a program needn't handle non-finite values. Where the reference program divides by a largest or mean magnitude, that divisor is 1e-20 or more.
Results may differ from the reference program's by a relative error of at most 0.001.
Values may be sent and summed in bfloat16 or wider, within the bound.
A program may use at most 128 MiB of HBM per device.

```python
import math
import jax
import jax.numpy as jnp
from jax import lax

D_MODEL = 2048
D_INNER = 8192


def raised(entries, stream_key, source, target, blocks, factor):
    owner, partner = [(jnp.arange(entries.shape[dim]) // (entries.shape[dim] // blocks)).reshape([-1 if axis == dim else 1 for axis in range(entries.ndim)]) for dim in (source, target)]
    chosen = jax.random.permutation(stream_key, blocks)[partner]
    strong = (owner == chosen) | (owner == (partner + blocks // 2) % blocks)
    return jnp.where(strong, factor * entries, entries)


def shard_levels(stream_key, dims, cuts, low, high):
    level, own = 1.0, jax.random.fold_in(stream_key, 6)
    for axis_at, blocks in cuts:
        draws = jnp.exp(jax.random.uniform(jax.random.fold_in(own, axis_at), (blocks,), jnp.float32, low / len(cuts), high / len(cuts)))
        level = level * jnp.repeat(draws, dims[axis_at] // blocks).reshape([-1 if axis == axis_at else 1 for axis in range(len(dims))])
    return level


def scatter_about(stream_key, shape, scale, most, shards=(), held_as=jnp.bfloat16):
    values = scale * jax.random.normal(stream_key, shape, jnp.float32)
    if shards:
        values = values * shard_levels(stream_key, shape, shards, -0.22, 0.18)
    return jnp.clip(values, -most, most).astype(held_as)


def heavy_noise(key, extent, width, limit, pieces, heavy, kind=jnp.bfloat16):
    entries = width * jax.random.normal(key, extent, jnp.float32)
    if pieces:
        entries = entries * shard_levels(key, extent, pieces, -0.22, 0.18)
    return jnp.clip(raised(entries, jax.random.fold_in(key, 3), *heavy), -limit, limit).astype(kind)


def setup_inputs(seed: int = 0) -> dict:
    arg_keys = jax.random.split(jax.random.key(seed), 9)
    weight_gate = heavy_noise(arg_keys[0], (D_MODEL, D_INNER), D_MODEL ** -0.5, 0.1875, ((0, 8), (1, 4)), (0, 1, 8, 2.0), jnp.float32)
    moment_gate = scatter_about(arg_keys[1], (D_MODEL, D_INNER), 1.0, 6.0, ((0, 8), (1, 4)), jnp.float32)
    square_gate = jnp.clip(jnp.exp(math.log(10.0) - 4.6051702 * jax.random.uniform(arg_keys[2], (D_MODEL, D_INNER), jnp.float32) ** shard_levels(arg_keys[2], (D_MODEL, D_INNER), ((0, 8), (1, 4)), -0.2, 0.2)), 0.1, 10.0)
    weight_up = heavy_noise(arg_keys[3], (D_MODEL, D_INNER), D_MODEL ** -0.5, 0.1875, ((0, 8), (1, 4)), (0, 1, 8, 2.0), jnp.float32)
    moment_up = scatter_about(arg_keys[4], (D_MODEL, D_INNER), 1.0, 6.0, ((0, 8), (1, 4)), jnp.float32)
    square_up = jnp.clip(jnp.exp(math.log(10.0) - 4.6051702 * jax.random.uniform(arg_keys[5], (D_MODEL, D_INNER), jnp.float32) ** shard_levels(arg_keys[5], (D_MODEL, D_INNER), ((0, 8), (1, 4)), -0.2, 0.2)), 0.1, 10.0)
    norm_train = jnp.clip(1.0 + 0.15 * jax.random.normal(arg_keys[6], (D_MODEL,), jnp.float32), 0.25, 1.75)
    norm_step = jnp.clip(jax.random.uniform(arg_keys[7], (D_MODEL,), jnp.float32, -0.3, 0.3) * shard_levels(arg_keys[7], (D_MODEL,), ((0, 32),), -0.4, 0.0), -0.3, 0.3)
    return dict(weight_gate=weight_gate, moment_gate=moment_gate, square_gate=square_gate, weight_up=weight_up, moment_up=moment_up, square_up=square_up, norm_train=norm_train, norm_step=norm_step)


learn_rate = 0.02
decay_rate = 0.1
tiny_value = 1e-08

def reference(weight_gate, moment_gate, square_gate, weight_up, moment_up, square_up, norm_train, norm_step):
    whole_gate = weight_gate - learn_rate * (moment_gate / (jnp.sqrt(square_gate) + tiny_value) + decay_rate * weight_gate)
    whole_up = weight_up - learn_rate * (moment_up / (jnp.sqrt(square_up) + tiny_value) + decay_rate * weight_up)
    scale_gate = lax.optimization_barrier(jnp.max(jnp.abs(whole_gate), axis=0))
    serving_gate = (whole_gate / scale_gate).astype(jnp.bfloat16)
    scale_up = lax.optimization_barrier(jnp.max(jnp.abs(whole_up), axis=0))
    serving_up = (whole_up / scale_up).astype(jnp.bfloat16)
    serve_norm = (norm_train + norm_step).astype(jnp.bfloat16)
    return (serving_gate, serving_up, scale_gate, scale_up, serve_norm, whole_gate, whole_up)
```

```python
import functools
import math

import jax
import jax.numpy as jnp
from jax import lax
from jax.experimental import pallas as pl
from jax.experimental.pallas import tpu as pltpu
from jax.sharding import PartitionSpec as P

MESH = pl.DeviceIdType.MESH
learn_rate = 0.02
decay_rate = 0.1
tiny_value = 1e-08
UNIT = 16
MOST = 9
LOAD = 32
BLOCK = 8
VMEM_LIMIT = 12 << 20


def gather_kernel(
    n, width, layers, group, rows, late_rows, a_count, k_count, count,
    wg, mg, sg, wu, mu, su, train, change,
    out, whole, scale_ref, norm,
    moment, square, mx, maxbuf, inv, terms, pieces, share, shares,
    in_sem, term_sem, ms, mr, ns1, nr1, ns2, nr2, zs, os, ys, rs,
):
    s, w = lax.axis_index("shard"), lax.axis_index("width")
    z, g = s // group, lax.rem(s, group)
    held, columns = wg.shape
    loads = held // LOAD
    parts = ((wg, whole), (mg, moment), (sg, square)), ((wu, whole), (mu, moment), (su, square))

    def load(m, i, c):
        source, target = parts[m][i]
        at = pl.multiple_of(c * LOAD, LOAD)
        return pltpu.make_async_copy(
            source.at[pl.ds(at, LOAD)], target.at[pl.ds(m * held + at, LOAD)], in_sem.at[m, i, c]
        )

    for m in range(2):
        @pl.loop(0, loads)
        def _(c):
            for i in range(3):
                load(m, i, c).start()

    term_loads = [
        pltpu.make_async_copy(ref, terms.at[i], term_sem.at[i]) for i, ref in enumerate((train, change))
    ]
    for term in term_loads:
        term.start()

    barrier = pltpu.get_barrier_semaphore()
    for j in range(1, n):
        pl.semaphore_signal(barrier, inc=1, device_id=(lax.rem(s + j, n), w), device_id_type=MESH)
    for j in range(1, width):
        pl.semaphore_signal(barrier, inc=1, device_id=(s, lax.rem(w + j, width)), device_id_type=MESH)

    def max_copy(m, j):
        return pltpu.make_async_remote_copy(
            mx.at[m], maxbuf.at[m, s], ms.at[m, j], mr.at[m, j],
            device_id=(lax.rem(s + j, n), w), device_id_type=MESH,
        )

    def piece_copy(j):
        return pltpu.make_async_remote_copy(
            pieces.at[w], pieces.at[w], ns1.at[j], nr1.at[j],
            device_id=(s, lax.rem(w + j, width)), device_id_type=MESH,
        )

    def norm_copy(j):
        return pltpu.make_async_remote_copy(
            shares.at[s], shares.at[s], ns2.at[j], nr2.at[j],
            device_id=(lax.rem(s + j, n), w), device_id_type=MESH,
        )

    def update(m):
        def chunk(c, top):
            for i in range(3):
                load(m, i, c).wait()

            def block(b, top):
                at = pl.ds(pl.multiple_of(m * held + c * LOAD + b * BLOCK, BLOCK), BLOCK)
                old = whole[at, :]
                new = old - learn_rate * (moment[at, :] / (jnp.sqrt(square[at, :]) + tiny_value) + decay_rate * old)
                whole[at, :] = new
                return jnp.maximum(top, jnp.abs(new))

            return lax.fori_loop(0, LOAD // BLOCK, block, top)

        top = lax.fori_loop(0, loads, chunk, jnp.zeros((BLOCK, columns), jnp.float32))
        mx[m] = jnp.max(top, axis=0, keepdims=True)

    def scale(m):
        for j in range(1, n):
            max_copy(m, j).wait_recv()
        top = mx[m]
        for j in range(1, n):
            top = jnp.maximum(top, maxbuf[m, lax.rem(s + n - j, n)])
        scale_ref[m] = top
        inv[m] = 1.0 / top

    update(0)
    lane = lax.broadcasted_iota(jnp.int32, (1, 128), 1)
    per = 128 // count
    spot = lax.rem(s * width + w, per)
    for term in term_loads:
        term.wait()
    piece = jnp.concatenate([terms[0] + terms[1]] * per, axis=1)
    pieces[w] = jnp.where(lane // count == spot, piece, 0.0)
    pl.semaphore_wait(barrier, n - 1 + width - 1)
    for j in range(1, n):
        max_copy(0, j).start()
    for j in range(1, width):
        piece_copy(j).start()
    update(1)
    for j in range(1, n):
        max_copy(1, j).start()
    for j in range(1, width):
        piece_copy(j).wait_recv()
    lines = max(1, width // per)
    for r in range(lines):
        total = pieces[r * (width // lines)]
        for i in range(1, width // lines):
            total = total + pieces[r * (width // lines) + i]
        share[r] = total
        shares[s, r] = total
    for j in range(1, n):
        norm_copy(j).start()

    def span(k):
        if isinstance(k, tuple):
            return pl.ds(pl.multiple_of(a_count * rows + k[0] * late_rows, UNIT), late_rows)
        return pl.ds(pl.multiple_of(k * rows, UNIT), rows)

    def slot(k):
        return a_count + k[0] if isinstance(k, tuple) else k

    def place(source, k):
        return out.at[source, span(k)]

    def copy(source, k, sem, device):
        return pltpu.make_async_remote_copy(
            place(source, k), place(source, k), sem, rs.at[source, slot(k)], device_id=(device, w), device_id_type=MESH
        )

    def partner(j):
        return z * group + lax.rem(g + j, group)

    def up(source, k, sem):
        return copy(source, k, sem.at[source, slot(k)], lax.rem(s + group, n))

    def down(source, k, sem):
        return copy(source, k, sem.at[source, slot(k)], lax.rem(s + n - group, n))

    def across(source, k, j):
        return copy(source, k, ys.at[j - 1, source, slot(k)], partner(j))

    def arrived(source, k):
        pltpu.make_async_copy(place(source, k), place(source, k), rs.at[source, slot(k)]).wait()

    def divide(m, unit):
        at = pl.ds(pl.multiple_of(unit * UNIT, UNIT), UNIT)
        out[s, at, :] = (whole[at, :] * inv[m]).astype(out.dtype)

    per_matrix = held // UNIT
    done = 0
    scale(0)

    def divide_to(limit):
        nonlocal done
        for m in range(2):
            first, last = max(done, m * per_matrix), min(limit, (m + 1) * per_matrix)
            if first < last:
                if m == 1 and done <= per_matrix:
                    scale(1)

                @pl.loop(first, last)
                def _(u):
                    divide(m, u)

                done = last

    for k in range(a_count):
        divide_to((k + 1) * rows // UNIT)

        @pl.when(z + 1 < layers)
        def _():
            up(s, k, zs).start()

        @pl.when(z > 0)
        def _():
            down(s, k, os).start()

        for j in range(1, group):
            across(s, k, j).start()

    divide_to(2 * held // UNIT)

    @pl.loop(0, k_count - a_count)
    def _(q):
        k = (q,)
        for j in range(1, group):
            across(s, k, j).start()

    for d in range(1, layers):
        @pl.loop(0, a_count)
        def _(k):
            @pl.when(z - d >= 0)
            def _():
                source = s - d * group
                arrived(source, k)

                @pl.when(z + 1 < layers)
                def _():
                    up(source, k, zs).start()

                for j in range(1, group):
                    across(source, k, j).start()

            @pl.when(z + d < layers)
            def _():
                source = s + d * group
                arrived(source, k)

                @pl.when(z > 0)
                def _():
                    down(source, k, zs).start()

                for j in range(1, group):
                    across(source, k, j).start()

    for j in range(group):
        source = partner(j)

        @pl.loop(0, k_count - a_count)
        def _(q):
            k = (q,)
            if j:
                arrived(source, k)

            @pl.when(z + 1 < layers)
            def _():
                up(source, k, zs).start()

            @pl.when(z > 0)
            def _():
                down(source, k, os).start()

    for d in range(1, layers):
        for j in range(group):
            @pl.loop(0, k_count - a_count)
            def _(q):
                k = (q,)

                @pl.when(z - d >= 0)
                def _():
                    source = partner(j) - d * group
                    arrived(source, k)

                    @pl.when(z + 1 < layers)
                    def _():
                        up(source, k, zs).start()

                @pl.when(z + d < layers)
                def _():
                    source = partner(j) + d * group
                    arrived(source, k)

                    @pl.when(z > 0)
                    def _():
                        down(source, k, zs).start()

    for j in range(1, group):
        @pl.loop(0, layers)
        def _(layer):
            @pl.loop(0, a_count)
            def _(k):
                arrived(layer * group + lax.rem(g + j, group), k)

    def left(source, k, layer):
        @pl.when((layer <= z) & (z + 1 < layers))
        def _():
            up(source, k, zs).wait_send()

        @pl.when((layer > z) & (z > 0))
        def _():
            down(source, k, zs).wait_send()

        @pl.when((layer == z) & (z > 0))
        def _():
            down(source, k, os).wait_send()

    @pl.loop(0, a_count)
    def _(k):

        @pl.loop(0, layers)
        def _(layer):
            source = layer * group + g
            left(source, k, layer)
            for j in range(1, group):
                across(source, k, j).wait_send()

    @pl.loop(0, k_count - a_count)
    def _(q):
        k = (q,)
        for j in range(1, group):
            across(s, k, j).wait_send()

        @pl.loop(0, layers)
        def _(layer):
            for j in range(group):
                left(layer * group + lax.rem(g + j, group), k, layer)

    for j in range(1, n):
        norm_copy(j).wait_recv()
    total_lines = norm.shape[0]
    for r in range(total_lines):
        if lines * n == total_lines:
            row = shares[r // lines, r % lines]
        else:
            many = n // total_lines
            row = shares[r * many, 0]
            for i in range(1, many):
                row = row + shares[r * many + i, 0]
        share[lines + r] = row
    norm[...] = share[pl.ds(lines, total_lines), 0, :].astype(norm.dtype)
    for j in range(1, width):
        piece_copy(j).wait_send()
    for j in range(1, n):
        max_copy(0, j).wait_send()
        max_copy(1, j).wait_send()
        norm_copy(j).wait_send()


def finish_kernel(n, out, whole, scale, norm, gate, up, whole_gate, whole_up, scale_gate, scale_up, serve, sem):
    held = whole.shape[0] // 2
    copies = []
    for i in range(n):
        for m, target in enumerate((gate, up)):
            copies.append((out.at[i, pl.ds(m * held, held)], target.at[pl.ds(i * held, held)]))
    for m, target in enumerate((whole_gate, whole_up)):
        copies.append((whole.at[pl.ds(m * held, held)], target))
    for m, target in enumerate((scale_gate, scale_up)):
        copies.append((scale.at[m], target))
    copies.append((norm, serve))
    copies = [pltpu.make_async_copy(a, b, sem.at[i]) for i, (a, b) in enumerate(copies)]
    for c in copies:
        c.start()
    for c in copies:
        c.wait()


def solution(mesh):
    n, width = mesh.shape["shard"], mesh.shape["width"]
    layers = math.gcd(n, math.isqrt(2 * n))
    group = n // layers

    def body(
        weight_gate, moment_gate, square_gate, weight_up, moment_up, square_up, norm_train, norm_step
    ):
        count = norm_train.shape[0]
        arrays = (
            weight_gate, moment_gate, square_gate, weight_up, moment_up, square_up,
            norm_train[None, :], norm_step[None, :],
        )
        held, columns = weight_gate.shape
        units = 2 * held // UNIT
        late_units = max(1, units * 5 // 32)
        early_units = units - late_units
        step = max(d for d in range(1, MOST + 1) if early_units % d == 0)
        rows, late_rows = step * UNIT, late_units * UNIT
        a_count, k_count = early_units // step, early_units // step + 1
        lines = max(1, width * count // 128)
        total_lines = n * width * count // 128
        loads = held // LOAD
        any_space = pl.BlockSpec(memory_space=pl.ANY)
        hbm_space = pl.BlockSpec(memory_space=pltpu.HBM)
        vmem_space = pl.BlockSpec(memory_space=pltpu.VMEM)
        dma = pltpu.SemaphoreType.DMA
        f32, bf16 = jnp.float32, jnp.bfloat16
        results = pl.pallas_call(
            functools.partial(
                gather_kernel, n, width, layers, group, rows, late_rows, a_count, k_count, count
            ),
            out_shape=(
                jax.ShapeDtypeStruct((n, 2 * held, columns), bf16),
                jax.ShapeDtypeStruct((2 * held, columns), f32),
                jax.ShapeDtypeStruct((2, 1, columns), f32),
                jax.ShapeDtypeStruct((total_lines, 128), bf16),
            ),
            in_specs=[hbm_space] * 8,
            out_specs=(vmem_space,) * 4,
            scratch_shapes=[
                pltpu.VMEM((2 * held, columns), f32),
                pltpu.VMEM((2 * held, columns), f32),
                pltpu.VMEM((2, 1, columns), f32),
                pltpu.VMEM((2, n, 1, columns), f32),
                pltpu.VMEM((2, 1, columns), f32),
                pltpu.VMEM((2, 1, count), f32),
                pltpu.VMEM((width, 1, 128), f32),
                pltpu.VMEM((lines + total_lines, 1, 128), f32),
                pltpu.VMEM((n, lines, 1, 128), f32),
                dma((2, 3, loads)),
                dma((2,)),
                dma((2, n)),
                dma((2, n)),
                dma((width,)),
                dma((width,)),
                dma((n,)),
                dma((n,)),
                dma((n, k_count)),
                dma((n, k_count)),
                dma((max(1, group - 1), n, k_count)),
                dma((n, k_count)),
            ],
            compiler_params=pltpu.CompilerParams(
                collective_id=0, has_side_effects=True, vmem_limit_bytes=VMEM_LIMIT
            ),
            name="gather",
        )(*(pltpu.with_memory_space_constraint(a, pltpu.HBM) for a in arrays))
        gate, up, whole_gate, whole_up, scale_gate, scale_up, serve = pl.pallas_call(
            functools.partial(finish_kernel, n),
            out_shape=(
                jax.ShapeDtypeStruct((n * held, columns), bf16),
                jax.ShapeDtypeStruct((n * held, columns), bf16),
                jax.ShapeDtypeStruct((held, columns), f32),
                jax.ShapeDtypeStruct((held, columns), f32),
                jax.ShapeDtypeStruct((1, columns), f32),
                jax.ShapeDtypeStruct((1, columns), f32),
                jax.ShapeDtypeStruct((total_lines, 128), bf16),
            ),
            in_specs=[any_space] * 4,
            out_specs=(hbm_space,) * 7,
            scratch_shapes=[dma((2 * n + 5,))],
            compiler_params=pltpu.CompilerParams(vmem_limit_bytes=1 << 20),
            name="finish",
        )(*results)
        return (
            gate, up, scale_gate.reshape(columns), scale_up.reshape(columns), serve.reshape(-1), whole_gate, whole_up
        )

    return jax.shard_map(
        body,
        mesh=mesh,
        in_specs=(P("shard", "width"),) * 6 + (P(("shard", "width")),) * 2,
        out_specs=(
            P(None, "width"),
            P(None, "width"),
            P("width"),
            P("width"),
            P(),
            P("shard", "width"),
            P("shard", "width"),
        ),
        check_vma=False,
    )
```

```python
import functools
import math

import jax
import jax.numpy as jnp
from jax import lax
from jax.experimental import pallas as pl
from jax.experimental.pallas import tpu as pltpu
from jax.sharding import PartitionSpec as P

MESH = pl.DeviceIdType.MESH
learn_rate = 0.02
decay_rate = 0.1
tiny_value = 1e-08
UNIT = 16
TILE = 8
RAW = 24
PARTS = 4
LOAD = 32
BLOCK = 8
VMEM_LIMIT = 12 << 20


def gather_kernel(
    n, width, layers, group, chunks, count,
    wg, mg, sg, wu, mu, su, train, change,
    out, whole, scale_ref, norm,
    moment, square, mx, maxbuf, inv, terms, pieces, share, shares, land,
    in_sem, term_sem, ms, mr, ns1, nr1, ns2, nr2, us, ds, ys, yr, zr, zl, es, er,
):
    s, w = lax.axis_index("shard"), lax.axis_index("width")
    z, g = s // group, lax.rem(s, group)
    above, below = lax.rem(s + group, n), lax.rem(s + n - group, n)
    raw = chunks[0][1]
    held, columns = wg.shape
    loads = held // LOAD
    parts = ((wg, whole), (mg, moment), (sg, square)), ((wu, whole), (mu, moment), (su, square))

    def load(m, i, c):
        source, target = parts[m][i]
        at = pl.multiple_of(c * LOAD, LOAD)
        return pltpu.make_async_copy(
            source.at[pl.ds(at, LOAD)], target.at[pl.ds(m * held + at, LOAD)], in_sem.at[m, c]
        )

    for i, ref in enumerate((train, change)):
        pltpu.make_async_copy(ref, terms.at[i], term_sem.at[0]).start()
    for m in range(2):
        @pl.loop(0, loads)
        def _(c):
            for i in range(3):
                load(m, i, c).start()

    barrier = pltpu.get_barrier_semaphore()
    for j in range(1, n):
        pl.semaphore_signal(barrier, inc=1, device_id=(lax.rem(s + j, n), w), device_id_type=MESH)
    for j in range(1, width):
        pl.semaphore_signal(barrier, inc=1, device_id=(s, lax.rem(w + j, width)), device_id_type=MESH)

    def max_copy(m, j):
        return pltpu.make_async_remote_copy(
            mx.at[m], maxbuf.at[m, s], ms.at[m], mr.at[m],
            device_id=(lax.rem(s + j, n), w), device_id_type=MESH,
        )

    def partner(j):
        return z * group + lax.rem(g + j, group)

    def raw_copy(lane):
        device = (above, below)[lane] if lane < 2 else partner(lane - 1)
        return pltpu.make_async_remote_copy(
            whole.at[pl.ds(0, raw)], land.at[lane], es.at[lane], er.at[lane],
            device_id=(device, w), device_id_type=MESH,
        )

    def piece_copy(j):
        return pltpu.make_async_remote_copy(
            pieces.at[w], pieces.at[w], ns1.at[0], nr1.at[0],
            device_id=(s, lax.rem(w + j, width)), device_id_type=MESH,
        )

    def norm_copy(j):
        return pltpu.make_async_remote_copy(
            shares.at[s], shares.at[s], ns2.at[0], nr2.at[0],
            device_id=(lax.rem(s + j, n), w), device_id_type=MESH,
        )

    trio = moment.at[pl.ds(0, 3 * LOAD)]

    def update(m):
        def chunk(c, top):
            pltpu.make_async_copy(trio, trio, in_sem.at[m, c]).wait()

            def block(b, top):
                at = pl.ds(pl.multiple_of(m * held + c * LOAD + b * BLOCK, BLOCK), BLOCK)
                old = whole[at, :]
                new = old - learn_rate * (moment[at, :] / (jnp.sqrt(square[at, :]) + tiny_value) + decay_rate * old)
                whole[at, :] = new
                return jnp.maximum(top, jnp.abs(new))

            return lax.fori_loop(0, LOAD // BLOCK, block, top)

        top = lax.fori_loop(0, loads, chunk, jnp.zeros((BLOCK, columns), jnp.float32))
        mx[m] = jnp.max(top, axis=0, keepdims=True)

    def scale(m):
        others = maxbuf.at[m, pl.ds(0, n - 1)]
        pltpu.make_async_copy(others, others, mr.at[m]).wait()
        top = mx[m]
        for j in range(1, n):
            top = jnp.maximum(top, maxbuf[m, lax.rem(s + n - j, n)])
        scale_ref[m] = top
        inv[m] = 1.0 / top

    update(0)
    lane = lax.broadcasted_iota(jnp.int32, (1, 128), 1)
    per = 128 // count
    spot = lax.rem(s * width + w, per)
    pltpu.make_async_copy(terms, terms, term_sem.at[0]).wait()
    piece = jnp.concatenate([terms[0] + terms[1]] * per, axis=1)
    pieces[w] = jnp.where(lane // count == spot, piece, 0.0)
    pl.semaphore_wait(barrier, n - 1 + width - 1)
    for j in range(1, n):
        max_copy(0, j).start()

    @pl.when(z + 1 < layers)
    def _():
        raw_copy(0).start()

    @pl.when(z > 0)
    def _():
        raw_copy(1).start()

    for j in range(1, group):
        raw_copy(1 + j).start()
    for j in range(1, width):
        piece_copy(j).start()
    update(1)
    for j in range(1, n):
        max_copy(1, j).start()
    last = len(chunks) - 1

    def place(source, k):
        start, size = chunks[k]
        return out.at[source, pl.ds(start, size)]

    def kind(k):
        return 0 if k == 0 else 2 if k == last else 1

    def copy(source, k, send, recv, device):
        return pltpu.make_async_remote_copy(
            place(source, k), place(source, k), send, recv, device_id=(device, w), device_id_type=MESH
        )

    def landed(source, k):
        return zl.at[source] if k == last else zr.at[source // group, k]

    def up(source, k):
        return copy(source, k, us.at[kind(k)], landed(source, k), above)

    def down(source, k):
        return copy(source, k, ds.at[kind(k)], landed(source, k), below)

    def across(source, k, j):
        recv = zl.at[source] if k == last else yr.at[j - 1, kind(k)]
        return copy(source, k, ys.at[j - 1, kind(k)], recv, partner(j))

    def across_all(source, k):
        for j in range(1, group):
            across(source, k, j).start()

    def arrived(source, k):
        pltpu.make_async_copy(place(source, k), place(source, k), landed(source, k)).wait()

    def settle(sem, many, size):
        block = out.at[pl.ds(0, many), pl.ds(0, size)]
        pltpu.make_async_copy(block, block, sem).wait()

    def divide(m, unit):
        at = pl.ds(pl.multiple_of(unit * UNIT, UNIT), UNIT)
        out[s, at, :] = (whole[at, :] * inv[m]).astype(out.dtype)

    per_matrix = held // UNIT
    done = 0
    scale(0)

    def divide_to(limit):
        nonlocal done
        for m in range(2):
            first, stop = max(done, m * per_matrix), min(limit, (m + 1) * per_matrix)
            if first < stop:
                if m == 1 and done <= per_matrix:
                    scale(1)

                @pl.loop(first, stop)
                def _(u):
                    divide(m, u)

                done = stop

    for k in range(1, last):
        divide_to(-(-sum(chunks[k]) // UNIT))

        @pl.when(z + 1 < layers)
        def _():
            up(s, k).start()

        @pl.when(z > 0)
        def _():
            down(s, k).start()

        across_all(s, k)

    divide_to(2 * held // UNIT)
    across_all(s, last)

    others = pieces.at[pl.ds(0, width - 1)]
    pltpu.make_async_copy(others, others, nr1.at[0]).wait()
    lines = max(1, width // per)
    for r in range(lines):
        total = pieces[r * (width // lines)]
        for i in range(1, width // lines):
            total = total + pieces[r * (width // lines) + i]
        share[r] = total
        shares[s, r] = total
    for j in range(1, n):
        norm_copy(j).start()

    def take(lane, source):
        raw_copy(lane).wait_recv()
        out[source, pl.ds(0, raw), :] = (land[lane] * inv[0]).astype(out.dtype)

    for d in range(1, layers):
        for k in range(last):
            @pl.when(z - d >= 0)
            def _():
                source = s - d * group
                take(0, source) if d == 1 and k == 0 else arrived(source, k)

                @pl.when(z + 1 < layers)
                def _():
                    up(source, k).start()

                across_all(source, k)

            @pl.when(z + d < layers)
            def _():
                source = s + d * group
                take(1, source) if d == 1 and k == 0 else arrived(source, k)

                @pl.when(z > 0)
                def _():
                    down(source, k).start()

                across_all(source, k)

            if d == 1 and k == 0:
                for j in range(1, group):
                    take(1 + j, partner(group - j))

    if layers == 1:
        for j in range(1, group):
            take(1 + j, partner(group - j))

    for j in range(group):
        source = partner(j)
        if j:
            arrived(source, last)

        @pl.when(z + 1 < layers)
        def _():
            up(source, last).start()

        @pl.when(z > 0)
        def _():
            down(source, last).start()

    for d in range(1, layers):
        for j in range(group):
            @pl.when(z - d >= 0)
            def _():
                source = partner(j) - d * group
                arrived(source, last)

                @pl.when(z + 1 < layers)
                def _():
                    up(source, last).start()

            @pl.when(z + d < layers)
            def _():
                source = partner(j) + d * group
                arrived(source, last)

                @pl.when(z > 0)
                def _():
                    down(source, last).start()

    early = sum(chunks[last - 1])
    tail = chunks[last][1]
    for sems in (yr, ys):
        for j in range(1, group):
            if layers > 1:
                settle(sems.at[j - 1, 0], layers - 1, raw)
            settle(sems.at[j - 1, 1], layers, early - raw)
    for j in range(1, group):
        settle(ys.at[j - 1, 2], 1, tail)
    for level in range(layers):
        @pl.when(z == level)
        def _():
            for sems, more, many in ((us, layers - 1 - level, level), (ds, level, layers - 1 - level)):
                if more:
                    if many:
                        settle(sems.at[0], many, raw)
                    settle(sems.at[1], many + 1, early - raw)
                    settle(sems.at[2], (many + 1) * group, tail)

    @pl.when(z + 1 < layers)
    def _():
        raw_copy(0).wait_send()

    @pl.when(z > 0)
    def _():
        raw_copy(1).wait_send()

    for j in range(1, group):
        raw_copy(1 + j).wait_send()

    others = shares.at[pl.ds(0, n - 1)]
    pltpu.make_async_copy(others, others, nr2.at[0]).wait()
    total_lines = norm.shape[0]
    for r in range(total_lines):
        if lines * n == total_lines:
            row = shares[r // lines, r % lines]
        else:
            many = n // total_lines
            row = shares[r * many, 0]
            for i in range(1, many):
                row = row + shares[r * many + i, 0]
        share[lines + r] = row
    norm[...] = share[pl.ds(lines, total_lines), 0, :].astype(norm.dtype)
    pltpu.make_async_copy(others, others, ns2.at[0]).wait()
    for m in range(2):
        block = maxbuf.at[m, pl.ds(0, n - 1)]
        pltpu.make_async_copy(block, block, ms.at[m]).wait()
    block = pieces.at[pl.ds(0, width - 1)]
    pltpu.make_async_copy(block, block, ns1.at[0]).wait()


def finish_kernel(out, whole, scale, norm, gate, up, whole_gate, whole_up, scale_gate, scale_up, serve, sem):
    held = whole.shape[0] // 2
    copies = []
    for m, target in enumerate((gate, up)):
        copies.append((out.at[:, pl.ds(m * held, held)], target))
    for m, target in enumerate((whole_gate, whole_up)):
        copies.append((whole.at[pl.ds(m * held, held)], target))
    for m, target in enumerate((scale_gate, scale_up)):
        copies.append((scale.at[m], target))
    copies.append((norm, serve))
    copies = [pltpu.make_async_copy(a, b, sem.at[i]) for i, (a, b) in enumerate(copies)]
    for c in copies:
        c.start()
    for c in copies:
        c.wait()


def solution(mesh):
    n, width = mesh.shape["shard"], mesh.shape["width"]
    layers = math.gcd(n, math.isqrt(2 * n))
    group = n // layers

    def body(
        weight_gate, moment_gate, square_gate, weight_up, moment_up, square_up, norm_train, norm_step
    ):
        count = norm_train.shape[0]
        arrays = (
            weight_gate, moment_gate, square_gate, weight_up, moment_up, square_up,
            norm_train[None, :], norm_step[None, :],
        )
        held, columns = weight_gate.shape
        late = -(-held // (3 * TILE)) * TILE
        early = 2 * held - late
        cuts = [0, RAW] + [early * i // (PARTS * TILE) * TILE for i in range(1, PARTS)] + [early, 2 * held]
        chunks = tuple((start, stop - start) for start, stop in zip(cuts, cuts[1:]))
        k_count = len(chunks)
        lines = max(1, width * count // 128)
        total_lines = n * width * count // 128
        loads = held // LOAD
        any_space = pl.BlockSpec(memory_space=pl.ANY)
        hbm_space = pl.BlockSpec(memory_space=pltpu.HBM)
        vmem_space = pl.BlockSpec(memory_space=pltpu.VMEM)
        dma = pltpu.SemaphoreType.DMA
        f32, bf16 = jnp.float32, jnp.bfloat16
        results = pl.pallas_call(
            functools.partial(
                gather_kernel, n, width, layers, group, chunks, count
            ),
            out_shape=(
                jax.ShapeDtypeStruct((n, 2 * held, columns), bf16),
                jax.ShapeDtypeStruct((2 * held, columns), f32),
                jax.ShapeDtypeStruct((2, 1, columns), f32),
                jax.ShapeDtypeStruct((total_lines, 128), bf16),
            ),
            in_specs=[hbm_space] * 8,
            out_specs=(vmem_space,) * 4,
            scratch_shapes=[
                pltpu.VMEM((2 * held, columns), f32),
                pltpu.VMEM((2 * held, columns), f32),
                pltpu.VMEM((2, 1, columns), f32),
                pltpu.VMEM((2, n, 1, columns), f32),
                pltpu.VMEM((2, 1, columns), f32),
                pltpu.VMEM((2, 1, count), f32),
                pltpu.VMEM((width, 1, 128), f32),
                pltpu.VMEM((lines + total_lines, 1, 128), f32),
                pltpu.VMEM((n, lines, 1, 128), f32),
                pltpu.VMEM((group + 1, RAW, columns), f32),
                dma((2, loads)),
                dma((1,)),
                dma((2,)),
                dma((2,)),
                dma((1,)),
                dma((1,)),
                dma((1,)),
                dma((1,)),
                dma((3,)),
                dma((3,)),
                dma((max(1, group - 1), 3)),
                dma((max(1, group - 1), 2)),
                dma((layers, k_count - 1)),
                dma((n,)),
                dma((group + 1,)),
                dma((group + 1,)),
            ],
            compiler_params=pltpu.CompilerParams(
                collective_id=0, has_side_effects=True, vmem_limit_bytes=VMEM_LIMIT
            ),
            name="gather",
        )(*(pltpu.with_memory_space_constraint(a, pltpu.HBM) for a in arrays))
        gate, up, whole_gate, whole_up, scale_gate, scale_up, serve = pl.pallas_call(
            finish_kernel,
            out_shape=(
                jax.ShapeDtypeStruct((n, held, columns), bf16),
                jax.ShapeDtypeStruct((n, held, columns), bf16),
                jax.ShapeDtypeStruct((held, columns), f32),
                jax.ShapeDtypeStruct((held, columns), f32),
                jax.ShapeDtypeStruct((1, columns), f32),
                jax.ShapeDtypeStruct((1, columns), f32),
                jax.ShapeDtypeStruct((total_lines, 128), bf16),
            ),
            in_specs=[any_space] * 4,
            out_specs=(hbm_space,) * 7,
            scratch_shapes=[dma((7,))],
            compiler_params=pltpu.CompilerParams(vmem_limit_bytes=1 << 20),
            name="finish",
        )(*results)
        return (
            gate.reshape(-1, columns), up.reshape(-1, columns), scale_gate.reshape(-1), scale_up.reshape(-1),
            serve.reshape(-1), whole_gate, whole_up,
        )

    return jax.shard_map(
        body,
        mesh=mesh,
        in_specs=(P("shard", "width"),) * 6 + (P(("shard", "width")),) * 2,
        out_specs=(
            P(None, "width"),
            P(None, "width"),
            P("width"),
            P("width"),
            P(),
            P("shard", "width"),
            P("shard", "width"),
        ),
        check_vma=False,
    )
```

```python
import functools
import math

import jax
import jax.numpy as jnp
from jax import lax
from jax.experimental import pallas as pl
from jax.experimental.pallas import tpu as pltpu
from jax.sharding import PartitionSpec as P

MESH = pl.DeviceIdType.MESH
learn_rate = 0.02
decay_rate = 0.1
tiny_value = 1e-08
UNIT = 16
TILE = 8
RAW = 32
ENDS = 40
SIDES = 64
PARTS = 2
SPLIT = 2
LOAD = 32
BLOCK = 8
VMEM_LIMIT = 12 << 20
FLOPS = 100_000_000


def gather_kernel(
    n, width, layers, group, chunks, hidden, count,
    wg, mg, sg, wu, mu, su, train, change,
    out, whole, scale_ref, norm, ends, sides,
    moment, square, mx, maxbuf, inv, terms, pieces, share, shares, land,
    in_sem, term_sem, ms, mr, ns1, nr1, ns2, nr2, us, ds, ys, yr, zr, zl, es, er,
):
    s, w = lax.axis_index("shard"), lax.axis_index("width")
    z, g = s // group, lax.rem(s, group)
    above, below = lax.rem(s + group, n), lax.rem(s + n - group, n)
    raw = chunks[0][1]
    held, columns = wg.shape
    half = columns // SPLIT
    trios = ((wg, whole), (mg, moment), (sg, square)), ((wu, whole), (mu, moment), (su, square))
    phases = [(0, i * half, half) for i in range(SPLIT)] + [(1, 0, columns)]

    def load(p, i, c):
        m, left, size = phases[p]
        source, target = trios[m][i]
        rows = LOAD * columns // size
        at = pl.multiple_of(c * rows, rows)
        cols = pl.ds(left, size)
        return pltpu.make_async_copy(
            source.at[pl.ds(at, rows), cols], target.at[pl.ds(m * held + at, rows), cols], in_sem.at[p, c]
        )

    def loads(p):
        return held * phases[p][2] // (LOAD * columns)

    for i, ref in enumerate((train, change)):
        pltpu.make_async_copy(ref, terms.at[i], term_sem.at[0]).start()
    for p in range(len(phases)):
        @pl.loop(0, loads(p))
        def _(c):
            for i in range(3):
                load(p, i, c).start()

    barrier = pltpu.get_barrier_semaphore()
    for j in range(1, n):
        pl.semaphore_signal(barrier, inc=1, device_id=(lax.rem(s + j, n), w), device_id_type=MESH)
    for j in range(1, width):
        pl.semaphore_signal(barrier, inc=1, device_id=(s, lax.rem(w + j, width)), device_id_type=MESH)

    def max_copy(p, j):
        m, left, size = phases[p]
        cols = pl.ds(left, size)
        return pltpu.make_async_remote_copy(
            mx.at[m, :, cols], maxbuf.at[m, s, :, cols], ms.at[0], mr.at[p],
            device_id=(lax.rem(s + j, n), w), device_id_type=MESH,
        )

    def max_send(p):
        for j in range(1, n):
            max_copy(p, j).start()

    def partner(j):
        return z * group + lax.rem(g + j, group)

    def raw_copy(lane):
        device = (above, below)[lane] if lane < 2 else partner(lane - 1)
        return pltpu.make_async_remote_copy(
            whole.at[pl.ds(0, raw), pl.ds(0, half)], land.at[lane], es.at[lane], er.at[lane],
            device_id=(device, w), device_id_type=MESH,
        )

    def piece_copy(j):
        return pltpu.make_async_remote_copy(
            pieces.at[w], pieces.at[w], ns1.at[0], nr1.at[0],
            device_id=(s, lax.rem(w + j, width)), device_id_type=MESH,
        )

    def norm_copy(j):
        return pltpu.make_async_remote_copy(
            shares.at[s], shares.at[s], ns2.at[0], nr2.at[0],
            device_id=(lax.rem(s + j, n), w), device_id_type=MESH,
        )

    trio = moment.at[pl.ds(0, 3 * LOAD)]

    def update(p):
        m, left, size = phases[p]
        cols = pl.ds(left, size)
        rows = LOAD * columns // size

        def chunk(c, top):
            pltpu.make_async_copy(trio, trio, in_sem.at[p, c]).wait()

            def block(b, top):
                at = pl.ds(pl.multiple_of(m * held + c * rows + b * BLOCK, BLOCK), BLOCK)
                old = whole[at, cols]
                new = old - learn_rate * (moment[at, cols] / (jnp.sqrt(square[at, cols]) + tiny_value) + decay_rate * old)
                whole[at, cols] = new
                return jnp.maximum(top, jnp.abs(new))

            return lax.fori_loop(0, rows // BLOCK, block, top)

        top = lax.fori_loop(0, loads(p), chunk, jnp.zeros((BLOCK, size), jnp.float32))
        mx[m, :, cols] = jnp.max(top, axis=0, keepdims=True)

    def scale(p):
        m, left, size = phases[p]
        cols = pl.ds(left, size)
        others = maxbuf.at[m, pl.ds(0, n - 1), :, cols]
        pltpu.make_async_copy(others, others, mr.at[p]).wait()
        top = mx[m, :, cols]
        for j in range(1, n):
            top = jnp.maximum(top, maxbuf[m, lax.rem(s + n - j, n), :, cols])
        scale_ref[m, :, cols] = top
        inv[m, :, cols] = 1.0 / top

    update(0)
    pl.semaphore_wait(barrier, n - 1 + width - 1)
    max_send(0)

    def raw_all(act):
        if raw:
            @pl.when(z + 1 < layers)
            def _():
                act(raw_copy(0))

            @pl.when(z > 0)
            def _():
                act(raw_copy(1))

            for j in range(1, group):
                act(raw_copy(1 + j))

    raw_all(lambda c: c.start())
    for p in range(1, SPLIT):
        update(p)
        max_send(p)
    lane = lax.broadcasted_iota(jnp.int32, (1, 128), 1)
    per = 128 // count
    spot = lax.rem(s * width + w, per)
    pltpu.make_async_copy(terms, terms, term_sem.at[0]).wait()
    piece = jnp.concatenate([terms[0] + terms[1]] * per, axis=1)
    pieces[w] = jnp.where(lane // count == spot, piece, 0.0)
    for j in range(1, width):
        piece_copy(j).start()

    late, tail = len(chunks) - 2, len(chunks) - 1
    side = late - 1 if hidden else -1
    lates = (late, tail) if hidden else (late,)

    def place(source, k):
        start, size, left, wide = chunks[k]
        return out.at[source, pl.ds(start, size), pl.ds(left, wide)]

    def kind(k):
        return 0 if k == 0 else 1 if k < late else k - late + 2

    def copy(source, k, send, recv, device):
        return pltpu.make_async_remote_copy(
            place(source, k), place(source, k), send, recv, device_id=(device, w), device_id_type=MESH
        )

    def landed(source, k):
        return zl.at[source, k - late] if k >= late else zr.at[source // group, k]

    def up(source, k):
        return copy(source, k, us.at[kind(k)], landed(source, k), above)

    def down(source, k):
        return copy(source, k, ds.at[kind(k)], landed(source, k), below)

    def across(source, k, j):
        spot = 4 if k == side else kind(k)
        recv = zl.at[source, k - late] if k >= late else yr.at[j - 1, spot]
        return copy(source, k, ys.at[j - 1, spot], recv, partner(j))

    def across_all(source, k):
        for j in range(1, group):
            across(source, k, j).start()

    def arrived(source, k):
        pltpu.make_async_copy(place(source, k), place(source, k), landed(source, k)).wait()

    def settle(sem, many, size):
        block = out.at[pl.ds(0, many), pl.ds(0, size)]
        pltpu.make_async_copy(block, block, sem).wait()

    def divide(start, stop, left, wide):
        m = start // held
        cols = pl.ds(left, wide)

        @pl.loop(start // UNIT, stop // UNIT)
        def _(u):
            at = pl.ds(pl.multiple_of(u * UNIT, UNIT), UNIT)
            out[s, at, cols] = (whole[at, cols] * inv[m, :, cols]).astype(out.dtype)

    def send(k):
        @pl.when(z + 1 < layers)
        def _():
            up(s, k).start()

        @pl.when(z > 0)
        def _():
            down(s, k).start()

        if k != side:
            across_all(s, k)

    done = held
    for k in range(1, late):
        start, size, left, wide = chunks[k]
        if start < held:
            scale(left // half)
            divide(0, held, left, wide)
            send(k)
            if k == 1:
                update(SPLIT)
                max_send(SPLIT)
        else:
            if done == held:
                scale(SPLIT)
            stop = -(-(start + size) // UNIT) * UNIT
            divide(done, stop, 0, columns)
            done = stop
            send(k)
    if done == held:
        scale(SPLIT)
    divide(done, 2 * held, 0, columns)
    for k in lates:
        across_all(s, k)
    if hidden:
        sides[...] = place(s, side)[...]
        ends[pl.ds(0, chunks[tail][1]), :] = place(s, tail)[...]

    others = pieces.at[pl.ds(0, width - 1)]
    pltpu.make_async_copy(others, others, nr1.at[0]).wait()
    lines = max(1, width // per)
    for r in range(lines):
        total = pieces[r * (width // lines)]
        for i in range(1, width // lines):
            total = total + pieces[r * (width // lines) + i]
        share[r] = total
        shares[s, r] = total
    for j in range(1, n):
        norm_copy(j).start()

    def take(lane, source):
        raw_copy(lane).wait_recv()
        cols = pl.ds(0, half)
        out[source, pl.ds(0, raw), cols] = (land[lane] * inv[0, :, cols]).astype(out.dtype)

    for d in range(1, layers):
        for k in range(0 if raw else 1, late):
            @pl.when(z - d >= 0)
            def _():
                source = s - d * group
                take(0, source) if d == 1 and k == 0 else arrived(source, k)

                @pl.when(z + 1 < layers)
                def _():
                    up(source, k).start()

                across_all(source, k)

            @pl.when(z + d < layers)
            def _():
                source = s + d * group
                take(1, source) if d == 1 and k == 0 else arrived(source, k)

                @pl.when(z > 0)
                def _():
                    down(source, k).start()

                across_all(source, k)

            if d == 1 and k == 0:
                for j in range(1, group):
                    take(1 + j, partner(group - j))

    if layers == 1 and raw:
        for j in range(1, group):
            take(1 + j, partner(group - j))

    for j in range(group):
        source = partner(j)
        for k in lates:
            if j:
                arrived(source, k)
            cut = 1 if k == tail else 0

            @pl.when(z + 1 + cut < layers)
            def _():
                up(source, k).start()

            @pl.when(z > cut)
            def _():
                down(source, k).start()

        if hidden and j:
            size = chunks[tail][1]
            ends[pl.ds(j * size, size), :] = place(source, tail)[...]

    for d in range(1, layers):
        for j in range(group):
            for k in lates:
                cut = 1 if k == tail and d == 1 else 0

                @pl.when((z - d >= 0) & (z + cut < layers))
                def _():
                    source = partner(j) - d * group
                    arrived(source, k)

                    @pl.when(z + 1 < layers)
                    def _():
                        up(source, k).start()

                @pl.when((z + d < layers) & (z >= cut))
                def _():
                    source = partner(j) + d * group
                    arrived(source, k)

                    @pl.when(z > 0)
                    def _():
                        down(source, k).start()

    early = chunks[late][0]
    plain = chunks[side][0] if hidden else early
    raw_lines = raw // SPLIT
    for sems in (yr, ys):
        for j in range(1, group):
            if layers > 1 and raw:
                settle(sems.at[j - 1, 0], layers - 1, raw_lines)
            settle(sems.at[j - 1, 1], layers, plain - raw_lines)
            if hidden:
                settle(sems.at[j - 1, 4], layers - 1, early - plain)
    for j in range(1, group):
        for k in lates:
            settle(ys.at[j - 1, kind(k)], 1, chunks[k][1])
    for level in range(layers):
        @pl.when(z == level)
        def _():
            for sems, more, many in ((us, layers - 1 - level, level), (ds, level, layers - 1 - level)):
                if more:
                    if many and raw:
                        settle(sems.at[0], many, raw_lines)
                    settle(sems.at[1], many + 1, early - raw_lines)
                    for k in lates:
                        own = 0 if k == tail and more == 1 else 1
                        if many + own:
                            settle(sems.at[kind(k)], (many + own) * group, chunks[k][1])

    raw_all(lambda c: c.wait_send())

    others = shares.at[pl.ds(0, n - 1)]
    pltpu.make_async_copy(others, others, nr2.at[0]).wait()
    total_lines = norm.shape[0]
    for r in range(total_lines):
        if lines * n == total_lines:
            row = shares[r // lines, r % lines]
        else:
            many = n // total_lines
            row = shares[r * many, 0]
            for i in range(1, many):
                row = row + shares[r * many + i, 0]
        share[lines + r] = row
    norm[...] = share[pl.ds(lines, total_lines), 0, :].astype(norm.dtype)
    pltpu.make_async_copy(others, others, ns2.at[0]).wait()
    block = maxbuf.at[:, pl.ds(0, n - 1)]
    pltpu.make_async_copy(block, block, ms.at[0]).wait()
    block = pieces.at[pl.ds(0, width - 1)]
    pltpu.make_async_copy(block, block, ns1.at[0]).wait()


def finish_kernel(out, whole, scale, norm, gate, up, whole_gate, whole_up, scale_gate, scale_up, serve, sem):
    held = whole.shape[0] // 2
    copies = []
    for m, target in enumerate((gate, up)):
        copies.append((out.at[:, pl.ds(m * held, held)], target))
    for m, target in enumerate((whole_gate, whole_up)):
        copies.append((whole.at[pl.ds(m * held, held)], target))
    for m, target in enumerate((scale_gate, scale_up)):
        copies.append((scale.at[m], target))
    copies.append((norm, serve))
    copies = [pltpu.make_async_copy(a, b, sem.at[i]) for i, (a, b) in enumerate(copies)]
    for c in copies:
        c.start()
    for c in copies:
        c.wait()


def patch_kernel(layers, group, at, far, near, _, up, sem):
    s = lax.axis_index("shard")
    z, g = s // group, lax.rem(s, group)
    partner = z * group + lax.rem(g + 1, group)
    rows, sides = far.shape[0] // group, near.shape[0]
    held = up.shape[1]
    copies = [pltpu.make_async_copy(near, up.at[partner, pl.ds(at, sides)], sem.at[0])]
    base = jnp.where(z == 0, 1, layers - 2) * group
    ends = [
        pltpu.make_async_copy(
            far.at[pl.ds(j * rows, rows)],
            up.at[base + lax.rem(g + j, group), pl.ds(held - rows, rows)],
            sem.at[1 + j],
        )
        for j in range(group)
    ]
    copies[0].start()

    @pl.when((z == 0) | (z == layers - 1))
    def _():
        for c in ends:
            c.start()
        for c in ends:
            c.wait()

    copies[0].wait()


def solution(mesh):
    n, width = mesh.shape["shard"], mesh.shape["width"]
    layers = math.gcd(n, math.isqrt(2 * n))
    group = n // layers

    def body(
        weight_gate, moment_gate, square_gate, weight_up, moment_up, square_up, norm_train, norm_step
    ):
        count = norm_train.shape[0]
        arrays = (
            weight_gate, moment_gate, square_gate, weight_up, moment_up, square_up,
            norm_train[None, :], norm_step[None, :],
        )
        held, columns = weight_gate.shape
        hidden = layers > 2 and group == 2
        late = -(-held // (3 * TILE)) * TILE
        early = 2 * held - late
        ends = min(ENDS, late // (2 * TILE) * TILE)
        half = columns // SPLIT
        chunks = [(0, RAW, 0, half), (RAW, held - RAW, 0, half)]
        chunks += [(0, held, i * half, half) for i in range(1, SPLIT)]
        stop = early - SIDES if hidden else early
        cuts = [held + (stop - held) * i // (PARTS * TILE) * TILE for i in range(PARTS)] + [stop]
        cuts += [early, 2 * held - ends, 2 * held] if hidden else [2 * held]
        chunks += [(start, stop - start, 0, columns) for start, stop in zip(cuts, cuts[1:])]
        if not hidden:
            chunks.append(chunks[-1])
        chunks = tuple(chunks)
        k_count = len(chunks)
        lines = max(1, width * count // 128)
        total_lines = n * width * count // 128
        any_space = pl.BlockSpec(memory_space=pl.ANY)
        hbm_space = pl.BlockSpec(memory_space=pltpu.HBM)
        vmem_space = pl.BlockSpec(memory_space=pltpu.VMEM)
        dma = pltpu.SemaphoreType.DMA
        f32, bf16 = jnp.float32, jnp.bfloat16
        results = pl.pallas_call(
            functools.partial(
                gather_kernel, n, width, layers, group, chunks, hidden, count
            ),
            out_shape=(
                jax.ShapeDtypeStruct((n, 2 * held, columns), bf16),
                jax.ShapeDtypeStruct((2 * held, columns), f32),
                jax.ShapeDtypeStruct((2, 1, columns), f32),
                jax.ShapeDtypeStruct((total_lines, 128), bf16),
                jax.ShapeDtypeStruct((group * ends, columns), bf16),
                jax.ShapeDtypeStruct((SIDES, columns), bf16),
            ),
            in_specs=[hbm_space] * 8,
            out_specs=(vmem_space,) * 6,
            scratch_shapes=[
                pltpu.VMEM((2 * held, columns), f32),
                pltpu.VMEM((2 * held, columns), f32),
                pltpu.VMEM((2, 1, columns), f32),
                pltpu.VMEM((2, n, 1, columns), f32),
                pltpu.VMEM((2, 1, columns), f32),
                pltpu.VMEM((2, 1, count), f32),
                pltpu.VMEM((width, 1, 128), f32),
                pltpu.VMEM((lines + total_lines, 1, 128), f32),
                pltpu.VMEM((n, lines, 1, 128), f32),
                pltpu.VMEM((group + 1, max(8, RAW), half), f32),
                dma((SPLIT + 1, held // LOAD)),
                dma((1,)),
                dma((1,)),
                dma((SPLIT + 1,)),
                dma((1,)),
                dma((1,)),
                dma((1,)),
                dma((1,)),
                dma((4,)),
                dma((4,)),
                dma((max(1, group - 1), 5)),
                dma((max(1, group - 1), 5)),
                dma((layers, k_count - 2)),
                dma((n, 2)),
                dma((group + 1,)),
                dma((group + 1,)),
            ],
            compiler_params=pltpu.CompilerParams(
                collective_id=0, has_side_effects=True, vmem_limit_bytes=VMEM_LIMIT
            ),
            name="gather",
        )(*(pltpu.with_memory_space_constraint(a, pltpu.HBM) for a in arrays))
        gate, up, whole_gate, whole_up, scale_gate, scale_up, serve = pl.pallas_call(
            finish_kernel,
            out_shape=(
                jax.ShapeDtypeStruct((n, held, columns), bf16),
                jax.ShapeDtypeStruct((n, held, columns), bf16),
                jax.ShapeDtypeStruct((held, columns), f32),
                jax.ShapeDtypeStruct((held, columns), f32),
                jax.ShapeDtypeStruct((1, columns), f32),
                jax.ShapeDtypeStruct((1, columns), f32),
                jax.ShapeDtypeStruct((total_lines, 128), bf16),
            ),
            in_specs=[any_space] * 4,
            out_specs=(hbm_space,) * 7,
            scratch_shapes=[dma((7,))],
            compiler_params=pltpu.CompilerParams(vmem_limit_bytes=1 << 20),
            cost_estimate=pl.CostEstimate(flops=FLOPS, bytes_accessed=0, transcendentals=0),
            name="finish",
        )(*results[:4])
        if hidden:
            inner = [(group, 0), ((layers - 2) * group, (layers - 1) * group)]
            ring = [(a + i, b + i) for a, b in inner for i in range(group)]
            swap = [(i, i + 1 - 2 * (i % 2)) for i in range(n)]
            far = lax.ppermute(results[4], "shard", ring)
            near = lax.ppermute(results[5], "shard", swap)
            up = pl.pallas_call(
                functools.partial(patch_kernel, layers, group, stop - held),
                out_shape=jax.ShapeDtypeStruct((n, held, columns), bf16),
                in_specs=[any_space] * 3,
                out_specs=any_space,
                scratch_shapes=[dma((3,))],
                input_output_aliases={2: 0},
                compiler_params=pltpu.CompilerParams(vmem_limit_bytes=1 << 20),
                name="patch",
            )(far, near, up)
        return (
            gate.reshape(-1, columns), up.reshape(-1, columns), scale_gate.reshape(-1), scale_up.reshape(-1),
            serve.reshape(-1), whole_gate, whole_up,
        )

    return jax.shard_map(
        body,
        mesh=mesh,
        in_specs=(P("shard", "width"),) * 6 + (P(("shard", "width")),) * 2,
        out_specs=(
            P(None, "width"),
            P(None, "width"),
            P("width"),
            P("width"),
            P(),
            P("shard", "width"),
            P("shard", "width"),
        ),
        check_vma=False,
    )
```

```python
import functools
import math

import jax
import jax.numpy as jnp
from jax import lax
from jax.experimental import pallas as pl
from jax.experimental.pallas import tpu as pltpu
from jax.sharding import PartitionSpec as P

MESH = pl.DeviceIdType.MESH
learn_rate = 0.02
decay_rate = 0.1
tiny_value = 1e-08
UNIT = 16
TILE = 8
RAW = 32
ENDS = 40
SIDES = 64
PARTS = 2
SPLIT = 2
LOAD = 32
BLOCK = 8
VMEM_LIMIT = 12 << 20
FLOPS = 100_000_000


def load_rows(held):
    return [min(SPLIT * LOAD, held)] * SPLIT + [min(2 * LOAD, held // 2)]


def gather_kernel(
    n, width, layers, group, chunks, hidden, count,
    wg, mg, sg, wu, mu, su, train, change,
    out, whole, scale_ref, norm, ends, sides,
    moment, square, mx, maxbuf, inv, linemax, terms, pieces, share, shares, land,
    in_sem, term_sem, ms, mr, ls, cs, mc, ns1, nr1, ns2, nr2, us, ds, ys, yr, zr, zl, es, er,
):
    s, w = lax.axis_index("shard"), lax.axis_index("width")
    z, g = s // group, lax.rem(s, group)
    above, below = lax.rem(s + group, n), lax.rem(s + n - group, n)
    raw = chunks[0][1]
    held, columns = wg.shape
    half = columns // SPLIT
    trios = ((wg, whole), (mg, moment), (sg, square)), ((wu, whole), (mu, moment), (su, square))
    phases = [(0, i * half, half) for i in range(SPLIT)] + [(1, 0, columns)]
    block_rows = load_rows(held)

    def load(p, i, c):
        m, left, size = phases[p]
        source, target = trios[m][i]
        rows = block_rows[p]
        at = pl.multiple_of(c * rows, rows)
        cols = pl.ds(left, size)
        return pltpu.make_async_copy(
            source.at[pl.ds(at, rows), cols], target.at[pl.ds(m * held + at, rows), cols], in_sem.at[p, c]
        )

    def loads(p):
        return held // block_rows[p]

    barrier = pltpu.get_barrier_semaphore()
    for j in range(1, n):
        pl.semaphore_signal(barrier, inc=1, device_id=(lax.rem(s + j, n), w), device_id_type=MESH)
    for j in range(1, width):
        pl.semaphore_signal(barrier, inc=1, device_id=(s, lax.rem(w + j, width)), device_id_type=MESH)

    for i, ref in enumerate((train, change)):
        pltpu.make_async_copy(ref, terms.at[i], term_sem.at[0]).start()
    for p in range(len(phases)):
        @pl.loop(0, loads(p))
        def _(c):
            for i in range(3):
                load(p, i, c).start()

    def max_copy(p, j):
        m, left, size = phases[p]
        cols = pl.ds(left, size)
        return pltpu.make_async_remote_copy(
            mx.at[m, :, cols], maxbuf.at[m, s, :, cols], ms.at[0], mr.at[p],
            device_id=(lax.rem(s + j, n), w), device_id_type=MESH,
        )

    def max_send(p):
        for j in range(1, n):
            max_copy(p, j).start()

    def line_peer(d):
        return lax.rem(z + d, layers) * group + g

    def line_send(p):
        m, left, size = phases[p]
        cols = pl.ds(left, size)
        for d in range(1, layers):
            pltpu.make_async_remote_copy(
                mx.at[m, :, cols], maxbuf.at[m, s, :, cols], ls.at[m], mr.at[p],
                device_id=(line_peer(d), w), device_id_type=MESH,
            ).start()

    def combine(p):
        m, left, size = phases[p]
        cols = pl.ds(left, size)
        top = mx[m, :, cols]
        if layers > 1:
            others = maxbuf.at[m, pl.ds(0, layers - 1), :, cols]
            pltpu.make_async_copy(others, others, mr.at[p]).wait()
            for d in range(1, layers):
                top = jnp.maximum(top, maxbuf[m, line_peer(d), :, cols])
        linemax[m, g, :, cols] = top
        for j in range(1, group):
            pltpu.make_async_remote_copy(
                linemax.at[m, g, :, cols], linemax.at[m, g, :, cols], cs.at[m], mc.at[p - 1],
                device_id=(partner(j), w), device_id_type=MESH,
            ).start()

    def partner(j):
        return z * group + lax.rem(g + j, group)

    def raw_copy(lane):
        device = (above, below)[lane] if lane < 2 else partner(lane - 1)
        return pltpu.make_async_remote_copy(
            whole.at[pl.ds(0, raw), pl.ds(0, half)], land.at[lane], es.at[lane], er.at[lane],
            device_id=(device, w), device_id_type=MESH,
        )

    def piece_copy(j):
        return pltpu.make_async_remote_copy(
            pieces.at[w], pieces.at[w], ns1.at[0], nr1.at[0],
            device_id=(s, lax.rem(w + j, width)), device_id_type=MESH,
        )

    def norm_copy(j):
        return pltpu.make_async_remote_copy(
            shares.at[s], shares.at[s], ns2.at[0], nr2.at[0],
            device_id=(lax.rem(s + j, n), w), device_id_type=MESH,
        )

    def update(p):
        m, left, size = phases[p]
        cols = pl.ds(left, size)
        rows = block_rows[p]
        trio = moment.at[pl.ds(0, 3 * rows * size // columns)]

        def chunk(c, top):
            pltpu.make_async_copy(trio, trio, in_sem.at[p, c]).wait()

            def block(b, top):
                at = pl.ds(pl.multiple_of(m * held + c * rows + b * BLOCK, BLOCK), BLOCK)
                old = whole[at, cols]
                new = old - learn_rate * (moment[at, cols] / (jnp.sqrt(square[at, cols]) + tiny_value) + decay_rate * old)
                whole[at, cols] = new
                return jnp.maximum(top, jnp.abs(new))

            return lax.fori_loop(0, rows // BLOCK, block, top)

        top = lax.fori_loop(0, loads(p), chunk, jnp.zeros((BLOCK, size), jnp.float32))
        mx[m, :, cols] = jnp.max(top, axis=0, keepdims=True)

    def scale(p):
        m, left, size = phases[p]
        cols = pl.ds(left, size)
        if p:
            others = linemax.at[m, pl.ds(0, group - 1), :, cols]
            pltpu.make_async_copy(others, others, mc.at[p - 1]).wait()
            top = linemax[m, 0, :, cols]
            for j in range(1, group):
                top = jnp.maximum(top, linemax[m, j, :, cols])
        else:
            others = maxbuf.at[m, pl.ds(0, n - 1), :, cols]
            pltpu.make_async_copy(others, others, mr.at[p]).wait()
            top = mx[m, :, cols]
            for j in range(1, n):
                top = jnp.maximum(top, maxbuf[m, lax.rem(s + n - j, n), :, cols])
        scale_ref[m, :, cols] = top
        inv[m, :, cols] = 1.0 / top

    update(0)
    pl.semaphore_wait(barrier, n - 1 + width - 1)
    max_send(0)

    def raw_all(act):
        if raw:
            @pl.when(z + 2 == layers)
            def _():
                act(raw_copy(0))

            @pl.when(z == 1)
            def _():
                act(raw_copy(1))

            for j in range(1, group):
                act(raw_copy(1 + j))

    raw_all(lambda c: c.start())
    for p in range(1, SPLIT + 1):
        update(p)
        line_send(p)
    lane = lax.broadcasted_iota(jnp.int32, (1, 128), 1)
    per = 128 // count
    spot = lax.rem(s * width + w, per)
    pltpu.make_async_copy(terms, terms, term_sem.at[0]).wait()
    piece = jnp.concatenate([terms[0] + terms[1]] * per, axis=1)
    pieces[w] = jnp.where(lane // count == spot, piece, 0.0)
    for j in range(1, width):
        piece_copy(j).start()

    late, tail = len(chunks) - 2, len(chunks) - 1
    side = late - 1 if hidden else -1
    lates = (late, tail) if hidden else (late,)

    def place(source, k):
        start, size, left, wide = chunks[k]
        return out.at[source, pl.ds(start, size), pl.ds(left, wide)]

    def kind(k):
        return 0 if k == 0 else 1 if k < late else k - late + 2

    def copy(source, k, send, recv, device):
        return pltpu.make_async_remote_copy(
            place(source, k), place(source, k), send, recv, device_id=(device, w), device_id_type=MESH
        )

    def landed(source, k, shift):
        return zl.at[source, k - late] if k >= late else zr.at[source // group - shift, k]

    def up(source, k):
        return copy(source, k, us.at[kind(k)], landed(source, k, 0), above)

    def down(source, k):
        return copy(source, k, ds.at[kind(k)], landed(source, k, 1), below)

    def across(source, k, j):
        spot = 4 if k == side else kind(k)
        recv = zl.at[source, k - late] if k >= late else yr.at[j - 1, spot]
        return copy(source, k, ys.at[j - 1, spot], recv, partner(j))

    def across_all(source, k):
        for j in range(1, group):
            across(source, k, j).start()

    def arrived(source, k, shift=0):
        pltpu.make_async_copy(place(source, k), place(source, k), landed(source, k, shift)).wait()

    def settle(sem, many, size):
        block = out.at[pl.ds(0, many), pl.ds(0, size)]
        pltpu.make_async_copy(block, block, sem).wait()

    def divide(start, stop, left, wide):
        m = start // held
        cols = pl.ds(left, wide)

        @pl.loop(start // UNIT, stop // UNIT)
        def _(u):
            at = pl.ds(pl.multiple_of(u * UNIT, UNIT), UNIT)
            out[s, at, cols] = (whole[at, cols] * inv[m, :, cols]).astype(out.dtype)

    def send(k):
        @pl.when(z + 1 < layers)
        def _():
            up(s, k).start()

        @pl.when(z > 0)
        def _():
            down(s, k).start()

        if k != side:
            across_all(s, k)

    done = held
    for k in range(1, late):
        start, size, left, wide = chunks[k]
        if start < held:
            if k == 1 or start == 0:
                scale(left // half)
                divide(0, held, left, wide)
            send(k)
            if k == 1:
                for p in range(1, SPLIT + 1):
                    combine(p)
                if raw:
                    @pl.when(z + 2 < layers)
                    def _():
                        up(s, 0).start()

                    @pl.when(z > 1)
                    def _():
                        down(s, 0).start()

        else:
            if done == held:
                scale(SPLIT)
            stop = -(-(start + size) // UNIT) * UNIT
            divide(done, stop, 0, columns)
            done = stop
            send(k)
    if done == held:
        scale(SPLIT)
    divide(done, 2 * held, 0, columns)
    for k in lates:
        across_all(s, k)
    if hidden:
        sides[...] = place(s, side)[...]
        ends[pl.ds(0, chunks[tail][1]), :] = place(s, tail)[...]

    others = pieces.at[pl.ds(0, width - 1)]
    pltpu.make_async_copy(others, others, nr1.at[0]).wait()
    lines = max(1, width // per)
    for r in range(lines):
        total = pieces[r * (width // lines)]
        for i in range(1, width // lines):
            total = total + pieces[r * (width // lines) + i]
        share[r] = total
        shares[s, r] = total
    for j in range(1, n):
        norm_copy(j).start()

    def take(lane, source):
        raw_copy(lane).wait_recv()
        cols = pl.ds(0, half)
        out[source, pl.ds(0, raw), cols] = (land[lane] * inv[0, :, cols]).astype(out.dtype)

    def receive(d, k, source, lane, end):
        if d == 1 and k == 0:
            @pl.when(end)
            def _():
                take(lane, source)

            @pl.when(jnp.logical_not(end))
            def _():
                arrived(source, k, lane)
        else:
            arrived(source, k, lane)

    for d in range(1, layers):
        for k in range(0 if raw else 1, late):
            @pl.when(z - d >= 0)
            def _():
                source = s - d * group
                receive(d, k, source, 0, z + 1 == layers)

                @pl.when(z + 1 < layers)
                def _():
                    up(source, k).start()

                across_all(source, k)

            @pl.when(z + d < layers)
            def _():
                source = s + d * group
                receive(d, k, source, 1, z == 0)

                @pl.when(z > 0)
                def _():
                    down(source, k).start()

                across_all(source, k)

            if d == 1 and k == 0:
                for j in range(1, group):
                    take(1 + j, partner(group - j))

    if layers == 1 and raw:
        for j in range(1, group):
            take(1 + j, partner(group - j))

    for j in range(group):
        source = partner(j)
        for k in lates:
            if j:
                arrived(source, k)
            cut = 1 if k == tail else 0

            @pl.when(z + 1 + cut < layers)
            def _():
                up(source, k).start()

            @pl.when(z > cut)
            def _():
                down(source, k).start()

        if hidden and j:
            size = chunks[tail][1]
            ends[pl.ds(j * size, size), :] = place(source, tail)[...]

    for d in range(1, layers):
        for j in range(group):
            for k in lates:
                cut = 1 if k == tail and d == 1 else 0

                @pl.when((z - d >= 0) & (z + cut < layers))
                def _():
                    source = partner(j) - d * group
                    arrived(source, k)

                    @pl.when(z + 1 < layers)
                    def _():
                        up(source, k).start()

                @pl.when((z + d < layers) & (z >= cut))
                def _():
                    source = partner(j) + d * group
                    arrived(source, k)

                    @pl.when(z > 0)
                    def _():
                        down(source, k).start()

    early = chunks[late][0]
    plain = chunks[side][0] if hidden else early
    raw_lines = raw // SPLIT
    for sems in (yr, ys):
        for j in range(1, group):
            if layers > 1 and raw:
                settle(sems.at[j - 1, 0], layers - 1, raw_lines)
            settle(sems.at[j - 1, 1], layers, plain - raw_lines)
            if hidden:
                settle(sems.at[j - 1, 4], layers - 1, early - plain)
    for j in range(1, group):
        for k in lates:
            settle(ys.at[j - 1, kind(k)], 1, chunks[k][1])
    for level in range(layers):
        @pl.when(z == level)
        def _():
            for sems, more, many in ((us, layers - 1 - level, level), (ds, level, layers - 1 - level)):
                if more:
                    own = 1 if more > 1 else 0
                    if many + own and raw:
                        settle(sems.at[0], many + own, raw_lines)
                    settle(sems.at[1], many + 1, early - raw_lines)
                    for k in lates:
                        own = 0 if k == tail and more == 1 else 1
                        if many + own:
                            settle(sems.at[kind(k)], (many + own) * group, chunks[k][1])

    raw_all(lambda c: c.wait_send())

    others = shares.at[pl.ds(0, n - 1)]
    pltpu.make_async_copy(others, others, nr2.at[0]).wait()
    total_lines = norm.shape[0]
    for r in range(total_lines):
        if lines * n == total_lines:
            row = shares[r // lines, r % lines]
        else:
            many = n // total_lines
            row = shares[r * many, 0]
            for i in range(1, many):
                row = row + shares[r * many + i, 0]
        share[lines + r] = row
    norm[...] = share[pl.ds(lines, total_lines), 0, :].astype(norm.dtype)
    pltpu.make_async_copy(others, others, ns2.at[0]).wait()
    block = maxbuf.at[0, pl.ds(0, n - 1), :, pl.ds(0, half)]
    pltpu.make_async_copy(block, block, ms.at[0]).wait()
    if layers > 1:
        for m, size in ((0, columns - half), (1, columns)):
            if size:
                block = maxbuf.at[m, pl.ds(0, layers - 1), :, pl.ds(0, size)]
                pltpu.make_async_copy(block, block, ls.at[m]).wait()
    for m, size in ((0, columns - half), (1, columns)):
        if size:
            block = linemax.at[m, pl.ds(0, group - 1), :, pl.ds(0, size)]
            pltpu.make_async_copy(block, block, cs.at[m]).wait()
    block = pieces.at[pl.ds(0, width - 1)]
    pltpu.make_async_copy(block, block, ns1.at[0]).wait()


def finish_kernel(out, whole, scale, norm, gate, up, whole_gate, whole_up, scale_gate, scale_up, serve, sem):
    held = whole.shape[0] // 2
    copies = []
    for m, target in enumerate((gate, up)):
        copies.append((out.at[:, pl.ds(m * held, held)], target))
    for m, target in enumerate((whole_gate, whole_up)):
        copies.append((whole.at[pl.ds(m * held, held)], target))
    for m, target in enumerate((scale_gate, scale_up)):
        copies.append((scale.at[m], target))
    copies.append((norm, serve))
    copies = [pltpu.make_async_copy(a, b, sem.at[i]) for i, (a, b) in enumerate(copies)]
    for c in copies:
        c.start()
    for c in copies:
        c.wait()


def patch_kernel(layers, group, at, far, near, _, up, sem):
    s = lax.axis_index("shard")
    z, g = s // group, lax.rem(s, group)
    partner = z * group + lax.rem(g + 1, group)
    rows, sides = far.shape[0] // group, near.shape[0]
    held = up.shape[1]
    copies = [pltpu.make_async_copy(near, up.at[partner, pl.ds(at, sides)], sem.at[0])]
    base = jnp.where(z == 0, 1, layers - 2) * group
    ends = [
        pltpu.make_async_copy(
            far.at[pl.ds(j * rows, rows)],
            up.at[base + lax.rem(g + j, group), pl.ds(held - rows, rows)],
            sem.at[1 + j],
        )
        for j in range(group)
    ]
    copies[0].start()

    @pl.when((z == 0) | (z == layers - 1))
    def _():
        for c in ends:
            c.start()
        for c in ends:
            c.wait()

    copies[0].wait()


def solution(mesh):
    n, width = mesh.shape["shard"], mesh.shape["width"]
    layers = math.gcd(n, math.isqrt(2 * n))
    group = n // layers

    def body(
        weight_gate, moment_gate, square_gate, weight_up, moment_up, square_up, norm_train, norm_step
    ):
        count = norm_train.shape[0]
        arrays = (
            weight_gate, moment_gate, square_gate, weight_up, moment_up, square_up,
            norm_train[None, :], norm_step[None, :],
        )
        held, columns = weight_gate.shape
        hidden = layers > 2 and group == 2
        late = -(-held // (3 * TILE)) * TILE
        early = 2 * held - late
        ends = min(ENDS, late // (2 * TILE) * TILE)
        half = columns // SPLIT
        chunks = [(0, RAW, 0, half), (RAW, held // 2 - RAW, 0, half), (held // 2, held - held // 2, 0, half)]
        chunks += [(0, held, i * half, half) for i in range(1, SPLIT)]
        stop = early - SIDES if hidden else early
        cuts = [held + (stop - held) * i // (PARTS * TILE) * TILE for i in range(PARTS)] + [stop]
        cuts += [early, 2 * held - ends, 2 * held] if hidden else [2 * held]
        chunks += [(start, stop - start, 0, columns) for start, stop in zip(cuts, cuts[1:])]
        if not hidden:
            chunks.append(chunks[-1])
        chunks = tuple(chunks)
        k_count = len(chunks)
        lines = max(1, width * count // 128)
        total_lines = n * width * count // 128
        any_space = pl.BlockSpec(memory_space=pl.ANY)
        hbm_space = pl.BlockSpec(memory_space=pltpu.HBM)
        vmem_space = pl.BlockSpec(memory_space=pltpu.VMEM)
        dma = pltpu.SemaphoreType.DMA
        f32, bf16 = jnp.float32, jnp.bfloat16
        results = pl.pallas_call(
            functools.partial(
                gather_kernel, n, width, layers, group, chunks, hidden, count
            ),
            out_shape=(
                jax.ShapeDtypeStruct((n, 2 * held, columns), bf16),
                jax.ShapeDtypeStruct((2 * held, columns), f32),
                jax.ShapeDtypeStruct((2, 1, columns), f32),
                jax.ShapeDtypeStruct((total_lines, 128), bf16),
                jax.ShapeDtypeStruct((group * ends, columns), bf16),
                jax.ShapeDtypeStruct((SIDES, columns), bf16),
            ),
            in_specs=[hbm_space] * 8,
            out_specs=(vmem_space,) * 6,
            scratch_shapes=[
                pltpu.VMEM((2 * held, columns), f32),
                pltpu.VMEM((2 * held, columns), f32),
                pltpu.VMEM((2, 1, columns), f32),
                pltpu.VMEM((2, n, 1, columns), f32),
                pltpu.VMEM((2, 1, columns), f32),
                pltpu.VMEM((2, group, 1, columns), f32),
                pltpu.VMEM((2, 1, count), f32),
                pltpu.VMEM((width, 1, 128), f32),
                pltpu.VMEM((lines + total_lines, 1, 128), f32),
                pltpu.VMEM((n, lines, 1, 128), f32),
                pltpu.VMEM((group + 1, max(8, RAW), half), f32),
                dma((SPLIT + 1, held // min(load_rows(held)))),
                dma((1,)),
                dma((1,)),
                dma((SPLIT + 1,)),
                dma((2,)),
                dma((2,)),
                dma((SPLIT,)),
                dma((1,)),
                dma((1,)),
                dma((1,)),
                dma((1,)),
                dma((4,)),
                dma((4,)),
                dma((max(1, group - 1), 5)),
                dma((max(1, group - 1), 5)),
                dma((max(1, layers - 1), k_count - 2)),
                dma((n, 2)),
                dma((group + 1,)),
                dma((group + 1,)),
            ],
            compiler_params=pltpu.CompilerParams(
                collective_id=0, has_side_effects=True, vmem_limit_bytes=VMEM_LIMIT
            ),
            name="gather",
        )(*(pltpu.with_memory_space_constraint(a, pltpu.HBM) for a in arrays))
        gate, up, whole_gate, whole_up, scale_gate, scale_up, serve = pl.pallas_call(
            finish_kernel,
            out_shape=(
                jax.ShapeDtypeStruct((n, held, columns), bf16),
                jax.ShapeDtypeStruct((n, held, columns), bf16),
                jax.ShapeDtypeStruct((held, columns), f32),
                jax.ShapeDtypeStruct((held, columns), f32),
                jax.ShapeDtypeStruct((1, columns), f32),
                jax.ShapeDtypeStruct((1, columns), f32),
                jax.ShapeDtypeStruct((total_lines, 128), bf16),
            ),
            in_specs=[any_space] * 4,
            out_specs=(hbm_space,) * 7,
            scratch_shapes=[dma((7,))],
            compiler_params=pltpu.CompilerParams(vmem_limit_bytes=1 << 20),
            cost_estimate=pl.CostEstimate(flops=FLOPS, bytes_accessed=0, transcendentals=0),
            name="finish",
        )(*results[:4])
        if hidden:
            inner = [(group, 0), ((layers - 2) * group, (layers - 1) * group)]
            ring = [(a + i, b + i) for a, b in inner for i in range(group)]
            swap = [(i, i + 1 - 2 * (i % 2)) for i in range(n)]
            far = lax.ppermute(results[4], "shard", ring)
            near = lax.ppermute(results[5], "shard", swap)
            up = pl.pallas_call(
                functools.partial(patch_kernel, layers, group, stop - held),
                out_shape=jax.ShapeDtypeStruct((n, held, columns), bf16),
                in_specs=[any_space] * 3,
                out_specs=any_space,
                scratch_shapes=[dma((3,))],
                input_output_aliases={2: 0},
                compiler_params=pltpu.CompilerParams(vmem_limit_bytes=1 << 20),
                name="patch",
            )(far, near, up)
        return (
            gate.reshape(-1, columns), up.reshape(-1, columns), scale_gate.reshape(-1), scale_up.reshape(-1),
            serve.reshape(-1), whole_gate, whole_up,
        )

    return jax.shard_map(
        body,
        mesh=mesh,
        in_specs=(P("shard", "width"),) * 6 + (P(("shard", "width")),) * 2,
        out_specs=(
            P(None, "width"),
            P(None, "width"),
            P("width"),
            P("width"),
            P(),
            P("shard", "width"),
            P("shard", "width"),
        ),
        check_vma=False,
    )
```

```python
import functools
import math

import jax
import jax.numpy as jnp
from jax import lax
from jax.experimental import pallas as pl
from jax.experimental.pallas import tpu as pltpu
from jax.sharding import PartitionSpec as P

MESH = pl.DeviceIdType.MESH
learn_rate = 0.02
decay_rate = 0.1
tiny_value = 1e-08
UNIT = 16
TILE = 8
RAW = 32
ENDS = 56
SIDES = 96
PARTS = 2
SPLIT = 2
LOAD = 32
BLOCK = 8
VMEM_LIMIT = 12 << 20
FLOPS = 100_000_000


def load_rows(held):
    return [min(SPLIT * LOAD, held)] * SPLIT + [min(2 * LOAD, held // 2)]


def gather_kernel(
    n, width, layers, group, chunks, hidden, count,
    wg, mg, sg, wu, mu, su, train, change,
    out, whole, scale_ref, norm, ends, sides,
    moment, square, mx, maxbuf, inv, linemax, terms, pieces, share, shares, land,
    in_sem, term_sem, ms, mr, ls, cs, mc, ns1, nr1, ns2, nr2, us, ds, ys, yr, zr, zl, es, er,
):
    s, w = lax.axis_index("shard"), lax.axis_index("width")
    z, g = s // group, lax.rem(s, group)
    above, below = lax.rem(s + group, n), lax.rem(s + n - group, n)
    raw = chunks[0][1]
    lead = lax.rem(w, 2) == 1
    rest = lax.rem(w, 2) == 0
    held, columns = wg.shape
    half = columns // SPLIT
    trios = ((wg, whole), (mg, moment), (sg, square)), ((wu, whole), (mu, moment), (su, square))
    phases = [(0, i * half, half) for i in range(SPLIT)] + [(1, 0, columns)]
    block_rows = load_rows(held)

    def load(p, i, c):
        m, left, size = phases[p]
        source, target = trios[m][i]
        rows = block_rows[p]
        at = pl.multiple_of(c * rows, rows)
        cols = pl.ds(left, size)
        return pltpu.make_async_copy(
            source.at[pl.ds(at, rows), cols], target.at[pl.ds(m * held + at, rows), cols], in_sem.at[p, c]
        )

    def loads(p):
        return held // block_rows[p]

    barrier = pltpu.get_barrier_semaphore()
    for j in range(1, n):
        pl.semaphore_signal(barrier, inc=1, device_id=(lax.rem(s + j, n), w), device_id_type=MESH)
    for j in range(1, width):
        pl.semaphore_signal(barrier, inc=1, device_id=(s, lax.rem(w + j, width)), device_id_type=MESH)

    for i, ref in enumerate((train, change)):
        pltpu.make_async_copy(ref, terms.at[i], term_sem.at[0]).start()
    for p in range(len(phases)):
        @pl.loop(0, loads(p))
        def _(c):
            for i in range(3):
                load(p, i, c).start()

    def max_copy(p, j):
        m, left, size = phases[p]
        cols = pl.ds(left, size)
        return pltpu.make_async_remote_copy(
            mx.at[m, :, cols], maxbuf.at[m, s, :, cols], ms.at[0], mr.at[p],
            device_id=(lax.rem(s + j, n), w), device_id_type=MESH,
        )

    def max_send(p):
        for j in range(1, n):
            max_copy(p, j).start()

    def line_peer(d):
        return lax.rem(z + d, layers) * group + g

    def line_send(p):
        m, left, size = phases[p]
        cols = pl.ds(left, size)
        for d in range(1, layers):
            pltpu.make_async_remote_copy(
                mx.at[m, :, cols], maxbuf.at[m, s, :, cols], ls.at[m], mr.at[p],
                device_id=(line_peer(d), w), device_id_type=MESH,
            ).start()

    def combine(p):
        m, left, size = phases[p]
        cols = pl.ds(left, size)
        top = mx[m, :, cols]
        if layers > 1:
            others = maxbuf.at[m, pl.ds(0, layers - 1), :, cols]
            pltpu.make_async_copy(others, others, mr.at[p]).wait()
            for d in range(1, layers):
                top = jnp.maximum(top, maxbuf[m, line_peer(d), :, cols])
        linemax[m, g, :, cols] = top
        for j in range(1, group):
            pltpu.make_async_remote_copy(
                linemax.at[m, g, :, cols], linemax.at[m, g, :, cols], cs.at[m], mc.at[p - 1],
                device_id=(partner(j), w), device_id_type=MESH,
            ).start()

    def partner(j):
        return z * group + lax.rem(g + j, group)

    def raw_copy(lane):
        device = (above, below)[lane] if lane < 2 else partner(lane - 1)
        return pltpu.make_async_remote_copy(
            whole.at[pl.ds(0, raw), pl.ds(0, half)], land.at[lane], es.at[lane], er.at[lane],
            device_id=(device, w), device_id_type=MESH,
        )

    def piece_copy(j):
        return pltpu.make_async_remote_copy(
            pieces.at[w], pieces.at[w], ns1.at[0], nr1.at[0],
            device_id=(s, lax.rem(w + j, width)), device_id_type=MESH,
        )

    def norm_copy(j):
        return pltpu.make_async_remote_copy(
            shares.at[s], shares.at[s], ns2.at[0], nr2.at[0],
            device_id=(lax.rem(s + j, n), w), device_id_type=MESH,
        )

    def update(p):
        m, left, size = phases[p]
        cols = pl.ds(left, size)
        rows = block_rows[p]
        trio = moment.at[pl.ds(0, 3 * rows * size // columns)]

        def chunk(c, top):
            pltpu.make_async_copy(trio, trio, in_sem.at[p, c]).wait()

            def block(b, top):
                at = pl.ds(pl.multiple_of(m * held + c * rows + b * BLOCK, BLOCK), BLOCK)
                old = whole[at, cols]
                new = old - learn_rate * (moment[at, cols] / (jnp.sqrt(square[at, cols]) + tiny_value) + decay_rate * old)
                whole[at, cols] = new
                return jnp.maximum(top, jnp.abs(new))

            return lax.fori_loop(0, rows // BLOCK, block, top)

        top = lax.fori_loop(0, loads(p), chunk, jnp.zeros((BLOCK, size), jnp.float32))
        mx[m, :, cols] = jnp.max(top, axis=0, keepdims=True)

    def scale(p):
        m, left, size = phases[p]
        cols = pl.ds(left, size)
        if p:
            others = linemax.at[m, pl.ds(0, group - 1), :, cols]
            pltpu.make_async_copy(others, others, mc.at[p - 1]).wait()
            top = linemax[m, 0, :, cols]
            for j in range(1, group):
                top = jnp.maximum(top, linemax[m, j, :, cols])
        else:
            others = maxbuf.at[m, pl.ds(0, n - 1), :, cols]
            pltpu.make_async_copy(others, others, mr.at[p]).wait()
            top = mx[m, :, cols]
            for j in range(1, n):
                top = jnp.maximum(top, maxbuf[m, lax.rem(s + n - j, n), :, cols])
        scale_ref[m, :, cols] = top
        inv[m, :, cols] = 1.0 / top

    update(0)
    pl.semaphore_wait(barrier, n - 1 + width - 1)
    max_send(0)

    def raw_all(act):
        if raw:
            @pl.when(z + 2 == layers)
            def _():
                act(raw_copy(0))

            @pl.when(z == 1)
            def _():
                act(raw_copy(1))

            for j in range(1, group):
                act(raw_copy(1 + j))

    raw_all(lambda c: c.start())
    for p in range(1, SPLIT + 1):
        update(p)
        line_send(p)
    lane = lax.broadcasted_iota(jnp.int32, (1, 128), 1)
    per = 128 // count
    spot = lax.rem(s * width + w, per)
    pltpu.make_async_copy(terms, terms, term_sem.at[0]).wait()
    piece = jnp.concatenate([terms[0] + terms[1]] * per, axis=1)
    pieces[w] = jnp.where(lane // count == spot, piece, 0.0)
    for j in range(1, width):
        piece_copy(j).start()

    late, tail = len(chunks) - 2, len(chunks) - 1
    side = late - 1 if hidden else -1
    lates = (late, tail) if hidden else (late,)

    def place(source, k):
        start, size, left, wide = chunks[k]
        return out.at[source, pl.ds(start, size), pl.ds(left, wide)]

    def kind(k):
        return 0 if k == 0 else 1 if k < late else k - late + 2

    def copy(source, k, send, recv, device):
        return pltpu.make_async_remote_copy(
            place(source, k), place(source, k), send, recv, device_id=(device, w), device_id_type=MESH
        )

    def landed(source, k, shift):
        return zl.at[source, k - late] if k >= late else zr.at[source // group - shift, k]

    def up(source, k):
        return copy(source, k, us.at[kind(k)], landed(source, k, 0), above)

    def down(source, k):
        return copy(source, k, ds.at[kind(k)], landed(source, k, 1), below)

    def across(source, k, j):
        spot = 4 if k == side else kind(k)
        recv = zl.at[source, k - late] if k >= late else yr.at[j - 1, spot]
        return copy(source, k, ys.at[j - 1, spot], recv, partner(j))

    def across_all(source, k):
        for j in range(1, group):
            across(source, k, j).start()

    def arrived(source, k, shift=0):
        pltpu.make_async_copy(place(source, k), place(source, k), landed(source, k, shift)).wait()

    def settle(sem, many, size):
        block = out.at[pl.ds(0, many), pl.ds(0, size)]
        pltpu.make_async_copy(block, block, sem).wait()

    def divide(start, stop, left, wide):
        m = start // held
        cols = pl.ds(left, wide)

        @pl.loop(start // UNIT, stop // UNIT)
        def _(u):
            at = pl.ds(pl.multiple_of(u * UNIT, UNIT), UNIT)
            out[s, at, cols] = (whole[at, cols] * inv[m, :, cols]).astype(out.dtype)

    def send(k):
        @pl.when(z + 1 < layers)
        def _():
            up(s, k).start()

        @pl.when(z > 0)
        def _():
            down(s, k).start()

        if k != side:
            across_all(s, k)

    done = held
    for k in range(1, late):
        start, size, left, wide = chunks[k]
        if start < held:
            if k == 1 or start == 0:
                scale(left // half)
                divide(0, held, left, wide)
            if k == 1:
                @pl.when(rest)
                def _():
                    for p in range(1, SPLIT + 1):
                        combine(p)

            send(k)
            if k == 1:
                @pl.when(lead)
                def _():
                    for p in range(1, SPLIT + 1):
                        combine(p)

                if raw:
                    @pl.when(z + 2 < layers)
                    def _():
                        up(s, 0).start()

                    @pl.when(z > 1)
                    def _():
                        down(s, 0).start()

        else:
            if done == held:
                scale(SPLIT)
            stop = -(-(start + size) // UNIT) * UNIT
            divide(done, stop, 0, columns)
            done = stop
            send(k)
    if done == held:
        scale(SPLIT)
    divide(done, 2 * held, 0, columns)
    for k in lates:
        across_all(s, k)
    if hidden:
        sides[...] = place(s, side)[...]
        ends[pl.ds(0, chunks[tail][1]), :] = place(s, tail)[...]

    others = pieces.at[pl.ds(0, width - 1)]
    pltpu.make_async_copy(others, others, nr1.at[0]).wait()
    lines = max(1, width // per)
    for r in range(lines):
        total = pieces[r * (width // lines)]
        for i in range(1, width // lines):
            total = total + pieces[r * (width // lines) + i]
        share[r] = total
        shares[s, r] = total
    for j in range(1, n):
        norm_copy(j).start()

    def take(lane, source):
        raw_copy(lane).wait_recv()
        cols = pl.ds(0, half)
        out[source, pl.ds(0, raw), cols] = (land[lane] * inv[0, :, cols]).astype(out.dtype)

    def receive(d, k, source, lane, end):
        if d == 1 and k == 0:
            @pl.when(end)
            def _():
                take(lane, source)

            @pl.when(jnp.logical_not(end))
            def _():
                arrived(source, k, lane)
        else:
            arrived(source, k, lane)

    for d in range(1, layers):
        for k in range(0 if raw else 1, late):
            @pl.when(z - d >= 0)
            def _():
                source = s - d * group
                receive(d, k, source, 0, z + 1 == layers)

                @pl.when(z + 1 < layers)
                def _():
                    up(source, k).start()

                across_all(source, k)

            @pl.when(z + d < layers)
            def _():
                source = s + d * group
                receive(d, k, source, 1, z == 0)

                @pl.when(z > 0)
                def _():
                    down(source, k).start()

                across_all(source, k)

            if d == 1 and k == 0:
                for j in range(1, group):
                    take(1 + j, partner(group - j))

    if layers == 1 and raw:
        for j in range(1, group):
            take(1 + j, partner(group - j))

    for j in range(group):
        source = partner(j)
        for k in lates:
            if j:
                arrived(source, k)
            cut = 1 if k == tail else 0

            @pl.when(z + 1 + cut < layers)
            def _():
                up(source, k).start()

            @pl.when(z > cut)
            def _():
                down(source, k).start()

        if hidden and j:
            size = chunks[tail][1]
            ends[pl.ds(j * size, size), :] = place(source, tail)[...]

    for d in range(1, layers):
        for j in range(group):
            for k in lates:
                cut = 1 if k == tail and d == 1 else 0

                @pl.when((z - d >= 0) & (z + cut < layers))
                def _():
                    source = partner(j) - d * group
                    arrived(source, k)

                    @pl.when(z + 1 < layers)
                    def _():
                        up(source, k).start()

                @pl.when((z + d < layers) & (z >= cut))
                def _():
                    source = partner(j) + d * group
                    arrived(source, k)

                    @pl.when(z > 0)
                    def _():
                        down(source, k).start()

    early = chunks[late][0]
    plain = chunks[side][0] if hidden else early
    raw_lines = raw // SPLIT
    for sems in (yr, ys):
        for j in range(1, group):
            if layers > 1 and raw:
                settle(sems.at[j - 1, 0], layers - 1, raw_lines)
            settle(sems.at[j - 1, 1], layers, plain - raw_lines)
            if hidden:
                settle(sems.at[j - 1, 4], layers - 1, early - plain)
    for j in range(1, group):
        for k in lates:
            settle(ys.at[j - 1, kind(k)], 1, chunks[k][1])
    for level in range(layers):
        @pl.when(z == level)
        def _():
            for sems, more, many in ((us, layers - 1 - level, level), (ds, level, layers - 1 - level)):
                if more:
                    own = 1 if more > 1 else 0
                    if many + own and raw:
                        settle(sems.at[0], many + own, raw_lines)
                    settle(sems.at[1], many + 1, early - raw_lines)
                    for k in lates:
                        own = 0 if k == tail and more == 1 else 1
                        if many + own:
                            settle(sems.at[kind(k)], (many + own) * group, chunks[k][1])

    raw_all(lambda c: c.wait_send())

    others = shares.at[pl.ds(0, n - 1)]
    pltpu.make_async_copy(others, others, nr2.at[0]).wait()
    total_lines = norm.shape[0]
    for r in range(total_lines):
        if lines * n == total_lines:
            row = shares[r // lines, r % lines]
        else:
            many = n // total_lines
            row = shares[r * many, 0]
            for i in range(1, many):
                row = row + shares[r * many + i, 0]
        share[lines + r] = row
    norm[...] = share[pl.ds(lines, total_lines), 0, :].astype(norm.dtype)
    pltpu.make_async_copy(others, others, ns2.at[0]).wait()
    block = maxbuf.at[0, pl.ds(0, n - 1), :, pl.ds(0, half)]
    pltpu.make_async_copy(block, block, ms.at[0]).wait()
    if layers > 1:
        for m, size in ((0, columns - half), (1, columns)):
            if size:
                block = maxbuf.at[m, pl.ds(0, layers - 1), :, pl.ds(0, size)]
                pltpu.make_async_copy(block, block, ls.at[m]).wait()
    for m, size in ((0, columns - half), (1, columns)):
        if size:
            block = linemax.at[m, pl.ds(0, group - 1), :, pl.ds(0, size)]
            pltpu.make_async_copy(block, block, cs.at[m]).wait()
    block = pieces.at[pl.ds(0, width - 1)]
    pltpu.make_async_copy(block, block, ns1.at[0]).wait()


def finish_kernel(out, whole, scale, norm, gate, up, whole_gate, whole_up, scale_gate, scale_up, serve, sem):
    held = whole.shape[0] // 2
    copies = []
    for m, target in enumerate((gate, up)):
        copies.append((out.at[:, pl.ds(m * held, held)], target))
    for m, target in enumerate((whole_gate, whole_up)):
        copies.append((whole.at[pl.ds(m * held, held)], target))
    for m, target in enumerate((scale_gate, scale_up)):
        copies.append((scale.at[m], target))
    copies.append((norm, serve))
    copies = [pltpu.make_async_copy(a, b, sem.at[i]) for i, (a, b) in enumerate(copies)]
    for c in copies:
        c.start()
    for c in copies:
        c.wait()


def patch_kernel(layers, group, at, far, near, _, up, sem):
    s = lax.axis_index("shard")
    z, g = s // group, lax.rem(s, group)
    partner = z * group + lax.rem(g + 1, group)
    rows, sides = far.shape[0] // group, near.shape[0]
    held = up.shape[1]
    copies = [pltpu.make_async_copy(near, up.at[partner, pl.ds(at, sides)], sem.at[0])]
    base = jnp.where(z == 0, 1, layers - 2) * group
    ends = [
        pltpu.make_async_copy(
            far.at[pl.ds(j * rows, rows)],
            up.at[base + lax.rem(g + j, group), pl.ds(held - rows, rows)],
            sem.at[1 + j],
        )
        for j in range(group)
    ]
    copies[0].start()

    @pl.when((z == 0) | (z == layers - 1))
    def _():
        for c in ends:
            c.start()
        for c in ends:
            c.wait()

    copies[0].wait()


def solution(mesh):
    n, width = mesh.shape["shard"], mesh.shape["width"]
    layers = math.gcd(n, math.isqrt(2 * n))
    group = n // layers

    def body(
        weight_gate, moment_gate, square_gate, weight_up, moment_up, square_up, norm_train, norm_step
    ):
        count = norm_train.shape[0]
        arrays = (
            weight_gate, moment_gate, square_gate, weight_up, moment_up, square_up,
            norm_train[None, :], norm_step[None, :],
        )
        held, columns = weight_gate.shape
        hidden = layers > 2 and group == 2
        late = -(-held // (3 * TILE)) * TILE
        early = 2 * held - late
        ends = min(ENDS, late - TILE)
        half = columns // SPLIT
        chunks = [(0, RAW, 0, half), (RAW, held // 2 - RAW, 0, half), (held // 2, held - held // 2, 0, half)]
        chunks += [(0, held, i * half, half) for i in range(1, SPLIT)]
        stop = early - SIDES if hidden else early
        cuts = [held + (stop - held) * i // (PARTS * TILE) * TILE for i in range(PARTS)] + [stop]
        cuts += [early, 2 * held - ends, 2 * held] if hidden else [2 * held]
        chunks += [(start, stop - start, 0, columns) for start, stop in zip(cuts, cuts[1:])]
        if not hidden:
            chunks.append(chunks[-1])
        chunks = tuple(chunks)
        k_count = len(chunks)
        lines = max(1, width * count // 128)
        total_lines = n * width * count // 128
        any_space = pl.BlockSpec(memory_space=pl.ANY)
        hbm_space = pl.BlockSpec(memory_space=pltpu.HBM)
        vmem_space = pl.BlockSpec(memory_space=pltpu.VMEM)
        dma = pltpu.SemaphoreType.DMA
        f32, bf16 = jnp.float32, jnp.bfloat16
        results = pl.pallas_call(
            functools.partial(
                gather_kernel, n, width, layers, group, chunks, hidden, count
            ),
            out_shape=(
                jax.ShapeDtypeStruct((n, 2 * held, columns), bf16),
                jax.ShapeDtypeStruct((2 * held, columns), f32),
                jax.ShapeDtypeStruct((2, 1, columns), f32),
                jax.ShapeDtypeStruct((total_lines, 128), bf16),
                jax.ShapeDtypeStruct((group * ends, columns), bf16),
                jax.ShapeDtypeStruct((SIDES, columns), bf16),
            ),
            in_specs=[hbm_space] * 8,
            out_specs=(vmem_space,) * 6,
            scratch_shapes=[
                pltpu.VMEM((2 * held, columns), f32),
                pltpu.VMEM((2 * held, columns), f32),
                pltpu.VMEM((2, 1, columns), f32),
                pltpu.VMEM((2, n, 1, columns), f32),
                pltpu.VMEM((2, 1, columns), f32),
                pltpu.VMEM((2, group, 1, columns), f32),
                pltpu.VMEM((2, 1, count), f32),
                pltpu.VMEM((width, 1, 128), f32),
                pltpu.VMEM((lines + total_lines, 1, 128), f32),
                pltpu.VMEM((n, lines, 1, 128), f32),
                pltpu.VMEM((group + 1, max(8, RAW), half), f32),
                dma((SPLIT + 1, held // min(load_rows(held)))),
                dma((1,)),
                dma((1,)),
                dma((SPLIT + 1,)),
                dma((2,)),
                dma((2,)),
                dma((SPLIT,)),
                dma((1,)),
                dma((1,)),
                dma((1,)),
                dma((1,)),
                dma((4,)),
                dma((4,)),
                dma((max(1, group - 1), 5)),
                dma((max(1, group - 1), 5)),
                dma((max(1, layers - 1), k_count - 2)),
                dma((n, 2)),
                dma((group + 1,)),
                dma((group + 1,)),
            ],
            compiler_params=pltpu.CompilerParams(
                collective_id=0, has_side_effects=True, vmem_limit_bytes=VMEM_LIMIT
            ),
            name="gather",
        )(*(pltpu.with_memory_space_constraint(a, pltpu.HBM) for a in arrays))
        gate, up, whole_gate, whole_up, scale_gate, scale_up, serve = pl.pallas_call(
            finish_kernel,
            out_shape=(
                jax.ShapeDtypeStruct((n, held, columns), bf16),
                jax.ShapeDtypeStruct((n, held, columns), bf16),
                jax.ShapeDtypeStruct((held, columns), f32),
                jax.ShapeDtypeStruct((held, columns), f32),
                jax.ShapeDtypeStruct((1, columns), f32),
                jax.ShapeDtypeStruct((1, columns), f32),
                jax.ShapeDtypeStruct((total_lines, 128), bf16),
            ),
            in_specs=[any_space] * 4,
            out_specs=(hbm_space,) * 7,
            scratch_shapes=[dma((7,))],
            compiler_params=pltpu.CompilerParams(vmem_limit_bytes=1 << 20),
            cost_estimate=pl.CostEstimate(flops=FLOPS, bytes_accessed=0, transcendentals=0),
            name="finish",
        )(*results[:4])
        if hidden:
            inner = [(group, 0), ((layers - 2) * group, (layers - 1) * group)]
            ring = [(a + i, b + i) for a, b in inner for i in range(group)]
            swap = [(i, i + 1 - 2 * (i % 2)) for i in range(n)]
            far = lax.ppermute(results[4], "shard", ring)
            near = lax.ppermute(results[5], "shard", swap)
            up = pl.pallas_call(
                functools.partial(patch_kernel, layers, group, stop - held),
                out_shape=jax.ShapeDtypeStruct((n, held, columns), bf16),
                in_specs=[any_space] * 3,
                out_specs=any_space,
                scratch_shapes=[dma((3,))],
                input_output_aliases={2: 0},
                compiler_params=pltpu.CompilerParams(vmem_limit_bytes=1 << 20),
                name="patch",
            )(far, near, up)
        return (
            gate.reshape(-1, columns), up.reshape(-1, columns), scale_gate.reshape(-1), scale_up.reshape(-1),
            serve.reshape(-1), whole_gate, whole_up,
        )

    return jax.shard_map(
        body,
        mesh=mesh,
        in_specs=(P("shard", "width"),) * 6 + (P(("shard", "width")),) * 2,
        out_specs=(
            P(None, "width"),
            P(None, "width"),
            P("width"),
            P("width"),
            P(),
            P("shard", "width"),
            P("shard", "width"),
        ),
        check_vma=False,
    )
```

```python
import functools
import math

import jax
import jax.numpy as jnp
from jax import lax
from jax.experimental import pallas as pl
from jax.experimental.pallas import tpu as pltpu
from jax.sharding import PartitionSpec as P

MESH = pl.DeviceIdType.MESH
learn_rate = 0.02
decay_rate = 0.1
tiny_value = 1e-08
UNIT = 16
TILE = 8
RAW = 32
ENDS = 56
SIDES = 104
PARTS = 2
SPLIT = 2
LOAD = 32
BLOCK = 8
VMEM_LIMIT = 12 << 20
FLOPS = 100_000_000


def load_rows(held):
    return [min(SPLIT * LOAD, held)] * SPLIT + [min(2 * LOAD, held // 2)]


def gather_kernel(
    n, width, layers, group, chunks, hidden, count,
    wg, mg, sg, wu, mu, su, train, change,
    out, whole, scale_ref, norm, ends, sides,
    moment, square, mx, maxbuf, inv, linemax, terms, pieces, share, shares, land,
    in_sem, term_sem, ms, mr, ls, cs, mc, ns1, nr1, ns2, nr2, us, ds, ys, yr, zr, zl, es, er,
):
    s, w = lax.axis_index("shard"), lax.axis_index("width")
    z, g = s // group, lax.rem(s, group)
    above, below = lax.rem(s + group, n), lax.rem(s + n - group, n)
    raw = chunks[0][1]
    lead = lax.rem(w, 2) == 1
    rest = lax.rem(w, 2) == 0
    held, columns = wg.shape
    half = columns // SPLIT
    trios = ((wg, whole), (mg, moment), (sg, square)), ((wu, whole), (mu, moment), (su, square))
    phases = [(0, i * half, half) for i in range(SPLIT)] + [(1, 0, columns)]
    block_rows = load_rows(held)

    def load(p, i, c):
        m, left, size = phases[p]
        source, target = trios[m][i]
        rows = block_rows[p]
        at = pl.multiple_of(c * rows, rows)
        cols = pl.ds(left, size)
        return pltpu.make_async_copy(
            source.at[pl.ds(at, rows), cols], target.at[pl.ds(m * held + at, rows), cols], in_sem.at[p, c]
        )

    def loads(p):
        return held // block_rows[p]

    barrier = pltpu.get_barrier_semaphore()
    for j in range(1, n):
        pl.semaphore_signal(barrier, inc=1, device_id=(lax.rem(s + j, n), w), device_id_type=MESH)
    for j in range(1, width):
        pl.semaphore_signal(barrier, inc=1, device_id=(s, lax.rem(w + j, width)), device_id_type=MESH)

    for i, ref in enumerate((train, change)):
        pltpu.make_async_copy(ref, terms.at[i], term_sem.at[0]).start()
    for p in range(len(phases)):
        @pl.loop(0, loads(p))
        def _(c):
            for i in range(3):
                load(p, i, c).start()

    def max_copy(p, j):
        m, left, size = phases[p]
        cols = pl.ds(left, size)
        return pltpu.make_async_remote_copy(
            mx.at[m, :, cols], maxbuf.at[m, s, :, cols], ms.at[0], mr.at[p],
            device_id=(lax.rem(s + j, n), w), device_id_type=MESH,
        )

    def max_send(p):
        for j in range(1, n):
            max_copy(p, j).start()

    def line_peer(d):
        return lax.rem(z + d, layers) * group + g

    def line_send(p):
        m, left, size = phases[p]
        cols = pl.ds(left, size)
        for d in range(1, layers):
            pltpu.make_async_remote_copy(
                mx.at[m, :, cols], maxbuf.at[m, s, :, cols], ls.at[m], mr.at[p],
                device_id=(line_peer(d), w), device_id_type=MESH,
            ).start()

    def combine(p):
        m, left, size = phases[p]
        cols = pl.ds(left, size)
        top = mx[m, :, cols]
        if layers > 1:
            others = maxbuf.at[m, pl.ds(0, layers - 1), :, cols]
            pltpu.make_async_copy(others, others, mr.at[p]).wait()
            for d in range(1, layers):
                top = jnp.maximum(top, maxbuf[m, line_peer(d), :, cols])
        linemax[m, g, :, cols] = top
        for j in range(1, group):
            pltpu.make_async_remote_copy(
                linemax.at[m, g, :, cols], linemax.at[m, g, :, cols], cs.at[m], mc.at[p - 1],
                device_id=(partner(j), w), device_id_type=MESH,
            ).start()

    def partner(j):
        return z * group + lax.rem(g + j, group)

    def raw_copy(lane):
        device = (above, below)[lane] if lane < 2 else partner(lane - 1)
        return pltpu.make_async_remote_copy(
            whole.at[pl.ds(0, raw), pl.ds(0, half)], land.at[lane], es.at[lane], er.at[lane],
            device_id=(device, w), device_id_type=MESH,
        )

    def piece_copy(j):
        return pltpu.make_async_remote_copy(
            pieces.at[w], pieces.at[w], ns1.at[0], nr1.at[0],
            device_id=(s, lax.rem(w + j, width)), device_id_type=MESH,
        )

    def norm_copy(j):
        return pltpu.make_async_remote_copy(
            shares.at[s], shares.at[s], ns2.at[0], nr2.at[0],
            device_id=(lax.rem(s + j, n), w), device_id_type=MESH,
        )

    def update(p):
        m, left, size = phases[p]
        cols = pl.ds(left, size)
        rows = block_rows[p]
        trio = moment.at[pl.ds(0, 3 * rows * size // columns)]

        def chunk(c, top):
            pltpu.make_async_copy(trio, trio, in_sem.at[p, c]).wait()

            def block(b, top):
                at = pl.ds(pl.multiple_of(m * held + c * rows + b * BLOCK, BLOCK), BLOCK)
                old = whole[at, cols]
                new = old - learn_rate * (moment[at, cols] / (jnp.sqrt(square[at, cols]) + tiny_value) + decay_rate * old)
                whole[at, cols] = new
                return jnp.maximum(top, jnp.abs(new))

            return lax.fori_loop(0, rows // BLOCK, block, top)

        top = lax.fori_loop(0, loads(p), chunk, jnp.zeros((BLOCK, size), jnp.float32))
        mx[m, :, cols] = jnp.max(top, axis=0, keepdims=True)

    def scale(p):
        m, left, size = phases[p]
        cols = pl.ds(left, size)
        if p:
            others = linemax.at[m, pl.ds(0, group - 1), :, cols]
            pltpu.make_async_copy(others, others, mc.at[p - 1]).wait()
            top = linemax[m, 0, :, cols]
            for j in range(1, group):
                top = jnp.maximum(top, linemax[m, j, :, cols])
        else:
            others = maxbuf.at[m, pl.ds(0, n - 1), :, cols]
            pltpu.make_async_copy(others, others, mr.at[p]).wait()
            top = mx[m, :, cols]
            for j in range(1, n):
                top = jnp.maximum(top, maxbuf[m, lax.rem(s + n - j, n), :, cols])
        scale_ref[m, :, cols] = top
        inv[m, :, cols] = 1.0 / top

    update(0)
    pl.semaphore_wait(barrier, n - 1 + width - 1)
    max_send(0)

    def raw_all(act):
        if raw:
            @pl.when(z + 2 == layers)
            def _():
                act(raw_copy(0))

            @pl.when(z == 1)
            def _():
                act(raw_copy(1))

            for j in range(1, group):
                act(raw_copy(1 + j))

    raw_all(lambda c: c.start())
    for p in range(1, SPLIT + 1):
        update(p)
        line_send(p)
    lane = lax.broadcasted_iota(jnp.int32, (1, 128), 1)
    per = 128 // count
    spot = lax.rem(s * width + w, per)
    pltpu.make_async_copy(terms, terms, term_sem.at[0]).wait()
    piece = jnp.concatenate([terms[0] + terms[1]] * per, axis=1)
    pieces[w] = jnp.where(lane // count == spot, piece, 0.0)
    for j in range(1, width):
        piece_copy(j).start()

    late, tail = len(chunks) - 2, len(chunks) - 1
    side = late - 1 if hidden else -1
    lates = (late, tail) if hidden else (late,)

    def place(source, k):
        start, size, left, wide = chunks[k]
        return out.at[source, pl.ds(start, size), pl.ds(left, wide)]

    def kind(k):
        return 0 if k == 0 else 1 if k < late else k - late + 2

    def copy(source, k, send, recv, device):
        return pltpu.make_async_remote_copy(
            place(source, k), place(source, k), send, recv, device_id=(device, w), device_id_type=MESH
        )

    def landed(source, k, shift):
        return zl.at[source, k - late] if k >= late else zr.at[source // group - shift, k]

    def up(source, k):
        return copy(source, k, us.at[kind(k)], landed(source, k, 0), above)

    def down(source, k):
        return copy(source, k, ds.at[kind(k)], landed(source, k, 1), below)

    def across(source, k, j):
        spot = 4 if k == side else kind(k)
        recv = zl.at[source, k - late] if k >= late else yr.at[j - 1, spot]
        return copy(source, k, ys.at[j - 1, spot], recv, partner(j))

    def across_all(source, k):
        for j in range(1, group):
            across(source, k, j).start()

    def arrived(source, k, shift=0):
        pltpu.make_async_copy(place(source, k), place(source, k), landed(source, k, shift)).wait()

    def settle(sem, many, size):
        block = out.at[pl.ds(0, many), pl.ds(0, size)]
        pltpu.make_async_copy(block, block, sem).wait()

    def divide(start, stop, left, wide):
        m = start // held
        cols = pl.ds(left, wide)

        @pl.loop(start // UNIT, stop // UNIT)
        def _(u):
            at = pl.ds(pl.multiple_of(u * UNIT, UNIT), UNIT)
            out[s, at, cols] = (whole[at, cols] * inv[m, :, cols]).astype(out.dtype)

    def send(k):
        @pl.when(z + 1 < layers)
        def _():
            up(s, k).start()

        @pl.when(z > 0)
        def _():
            down(s, k).start()

        if k != side:
            across_all(s, k)

    done = held
    for k in range(1, late):
        start, size, left, wide = chunks[k]
        if start < held:
            if k == 1 or start == 0:
                scale(left // half)
                divide(0, held, left, wide)
            if k == 1:
                @pl.when(rest)
                def _():
                    for p in range(1, SPLIT + 1):
                        combine(p)

            send(k)
            if k == 1:
                @pl.when(lead)
                def _():
                    for p in range(1, SPLIT + 1):
                        combine(p)

                if raw:
                    @pl.when(z + 2 < layers)
                    def _():
                        up(s, 0).start()

                    @pl.when(z > 1)
                    def _():
                        down(s, 0).start()

        else:
            if done == held:
                scale(SPLIT)
            stop = -(-(start + size) // UNIT) * UNIT
            divide(done, stop, 0, columns)
            done = stop
            send(k)
    if done == held:
        scale(SPLIT)
    divide(done, 2 * held, 0, columns)
    for k in lates:
        across_all(s, k)
    if hidden:
        sides[...] = place(s, side)[...]
        ends[pl.ds(0, chunks[tail][1]), :] = place(s, tail)[...]

    others = pieces.at[pl.ds(0, width - 1)]
    pltpu.make_async_copy(others, others, nr1.at[0]).wait()
    lines = max(1, width // per)
    for r in range(lines):
        total = pieces[r * (width // lines)]
        for i in range(1, width // lines):
            total = total + pieces[r * (width // lines) + i]
        share[r] = total
        shares[s, r] = total
    for j in range(1, n):
        norm_copy(j).start()

    def take(lane, source):
        raw_copy(lane).wait_recv()
        cols = pl.ds(0, half)
        out[source, pl.ds(0, raw), cols] = (land[lane] * inv[0, :, cols]).astype(out.dtype)

    def receive(d, k, source, lane, end):
        if d == 1 and k == 0:
            @pl.when(end)
            def _():
                take(lane, source)

            @pl.when(jnp.logical_not(end))
            def _():
                arrived(source, k, lane)
        else:
            arrived(source, k, lane)

    for d in range(1, layers):
        for k in range(0 if raw else 1, late):
            @pl.when(z - d >= 0)
            def _():
                source = s - d * group
                receive(d, k, source, 0, z + 1 == layers)

                @pl.when(z + 1 < layers)
                def _():
                    up(source, k).start()

                across_all(source, k)

            @pl.when(z + d < layers)
            def _():
                source = s + d * group
                receive(d, k, source, 1, z == 0)

                @pl.when(z > 0)
                def _():
                    down(source, k).start()

                across_all(source, k)

            if d == 1 and k == 0:
                for j in range(1, group):
                    take(1 + j, partner(group - j))

    if layers == 1 and raw:
        for j in range(1, group):
            take(1 + j, partner(group - j))

    for j in range(group):
        source = partner(j)
        for k in lates:
            if j:
                arrived(source, k)
            cut = 1 if k == tail else 0

            @pl.when(z + 1 + cut < layers)
            def _():
                up(source, k).start()

            @pl.when(z > cut)
            def _():
                down(source, k).start()

        if hidden and j:
            size = chunks[tail][1]
            ends[pl.ds(j * size, size), :] = place(source, tail)[...]

    for d in range(1, layers):
        for j in range(group):
            for k in lates:
                cut = 1 if k == tail and d == 1 else 0

                @pl.when((z - d >= 0) & (z + cut < layers))
                def _():
                    source = partner(j) - d * group
                    arrived(source, k)

                    @pl.when(z + 1 < layers)
                    def _():
                        up(source, k).start()

                @pl.when((z + d < layers) & (z >= cut))
                def _():
                    source = partner(j) + d * group
                    arrived(source, k)

                    @pl.when(z > 0)
                    def _():
                        down(source, k).start()

    early = chunks[late][0]
    plain = chunks[side][0] if hidden else early
    raw_lines = raw // SPLIT
    for sems in (yr, ys):
        for j in range(1, group):
            if layers > 1 and raw:
                settle(sems.at[j - 1, 0], layers - 1, raw_lines)
            settle(sems.at[j - 1, 1], layers, plain - raw_lines)
            if hidden:
                settle(sems.at[j - 1, 4], layers - 1, early - plain)
    for j in range(1, group):
        for k in lates:
            settle(ys.at[j - 1, kind(k)], 1, chunks[k][1])
    for level in range(layers):
        @pl.when(z == level)
        def _():
            for sems, more, many in ((us, layers - 1 - level, level), (ds, level, layers - 1 - level)):
                if more:
                    own = 1 if more > 1 else 0
                    if many + own and raw:
                        settle(sems.at[0], many + own, raw_lines)
                    settle(sems.at[1], many + 1, early - raw_lines)
                    for k in lates:
                        own = 0 if k == tail and more == 1 else 1
                        if many + own:
                            settle(sems.at[kind(k)], (many + own) * group, chunks[k][1])

    raw_all(lambda c: c.wait_send())

    others = shares.at[pl.ds(0, n - 1)]
    pltpu.make_async_copy(others, others, nr2.at[0]).wait()
    total_lines = norm.shape[0]
    for r in range(total_lines):
        if lines * n == total_lines:
            row = shares[r // lines, r % lines]
        else:
            many = n // total_lines
            row = shares[r * many, 0]
            for i in range(1, many):
                row = row + shares[r * many + i, 0]
        share[lines + r] = row
    norm[...] = share[pl.ds(lines, total_lines), 0, :].astype(norm.dtype)
    pltpu.make_async_copy(others, others, ns2.at[0]).wait()
    block = maxbuf.at[0, pl.ds(0, n - 1), :, pl.ds(0, half)]
    pltpu.make_async_copy(block, block, ms.at[0]).wait()
    if layers > 1:
        for m, size in ((0, columns - half), (1, columns)):
            if size:
                block = maxbuf.at[m, pl.ds(0, layers - 1), :, pl.ds(0, size)]
                pltpu.make_async_copy(block, block, ls.at[m]).wait()
    for m, size in ((0, columns - half), (1, columns)):
        if size:
            block = linemax.at[m, pl.ds(0, group - 1), :, pl.ds(0, size)]
            pltpu.make_async_copy(block, block, cs.at[m]).wait()
    block = pieces.at[pl.ds(0, width - 1)]
    pltpu.make_async_copy(block, block, ns1.at[0]).wait()


def finish_kernel(out, whole, scale, norm, gate, up, whole_gate, whole_up, scale_gate, scale_up, serve, sem):
    held = whole.shape[0] // 2
    copies = []
    for m, target in enumerate((gate, up)):
        copies.append((out.at[:, pl.ds(m * held, held)], target))
    for m, target in enumerate((whole_gate, whole_up)):
        copies.append((whole.at[pl.ds(m * held, held)], target))
    for m, target in enumerate((scale_gate, scale_up)):
        copies.append((scale.at[m], target))
    copies.append((norm, serve))
    copies = [pltpu.make_async_copy(a, b, sem.at[i]) for i, (a, b) in enumerate(copies)]
    for c in copies:
        c.start()
    for c in copies:
        c.wait()


def patch_kernel(layers, group, at, far, near, _, up, sem):
    s = lax.axis_index("shard")
    z, g = s // group, lax.rem(s, group)
    partner = z * group + lax.rem(g + 1, group)
    rows, sides = far.shape[0] // group, near.shape[0]
    held = up.shape[1]
    copies = [pltpu.make_async_copy(near, up.at[partner, pl.ds(at, sides)], sem.at[0])]
    base = jnp.where(z == 0, 1, layers - 2) * group
    ends = [
        pltpu.make_async_copy(
            far.at[pl.ds(j * rows, rows)],
            up.at[base + lax.rem(g + j, group), pl.ds(held - rows, rows)],
            sem.at[1 + j],
        )
        for j in range(group)
    ]
    copies[0].start()

    @pl.when((z == 0) | (z == layers - 1))
    def _():
        for c in ends:
            c.start()
        for c in ends:
            c.wait()

    copies[0].wait()


def solution(mesh):
    n, width = mesh.shape["shard"], mesh.shape["width"]
    layers = math.gcd(n, math.isqrt(2 * n))
    group = n // layers

    def body(
        weight_gate, moment_gate, square_gate, weight_up, moment_up, square_up, norm_train, norm_step
    ):
        count = norm_train.shape[0]
        arrays = (
            weight_gate, moment_gate, square_gate, weight_up, moment_up, square_up,
            norm_train[None, :], norm_step[None, :],
        )
        held, columns = weight_gate.shape
        hidden = layers > 2 and group == 2
        late = -(-held // (3 * TILE)) * TILE
        early = 2 * held - late
        ends = min(ENDS, late - TILE)
        half = columns // SPLIT
        chunks = [(0, RAW, 0, half), (RAW, held // 2 - RAW, 0, half), (held // 2, held - held // 2, 0, half)]
        chunks += [(0, held, i * half, half) for i in range(1, SPLIT)]
        stop = early - SIDES if hidden else early
        cuts = [held + (stop - held) * i // (PARTS * TILE) * TILE for i in range(PARTS)] + [stop]
        cuts += [early, 2 * held - ends, 2 * held] if hidden else [2 * held]
        chunks += [(start, stop - start, 0, columns) for start, stop in zip(cuts, cuts[1:])]
        if not hidden:
            chunks.append(chunks[-1])
        chunks = tuple(chunks)
        k_count = len(chunks)
        lines = max(1, width * count // 128)
        total_lines = n * width * count // 128
        any_space = pl.BlockSpec(memory_space=pl.ANY)
        hbm_space = pl.BlockSpec(memory_space=pltpu.HBM)
        vmem_space = pl.BlockSpec(memory_space=pltpu.VMEM)
        dma = pltpu.SemaphoreType.DMA
        f32, bf16 = jnp.float32, jnp.bfloat16
        results = pl.pallas_call(
            functools.partial(
                gather_kernel, n, width, layers, group, chunks, hidden, count
            ),
            out_shape=(
                jax.ShapeDtypeStruct((n, 2 * held, columns), bf16),
                jax.ShapeDtypeStruct((2 * held, columns), f32),
                jax.ShapeDtypeStruct((2, 1, columns), f32),
                jax.ShapeDtypeStruct((total_lines, 128), bf16),
                jax.ShapeDtypeStruct((group * ends, columns), bf16),
                jax.ShapeDtypeStruct((SIDES, columns), bf16),
            ),
            in_specs=[hbm_space] * 8,
            out_specs=(vmem_space,) * 6,
            scratch_shapes=[
                pltpu.VMEM((2 * held, columns), f32),
                pltpu.VMEM((2 * held, columns), f32),
                pltpu.VMEM((2, 1, columns), f32),
                pltpu.VMEM((2, n, 1, columns), f32),
                pltpu.VMEM((2, 1, columns), f32),
                pltpu.VMEM((2, group, 1, columns), f32),
                pltpu.VMEM((2, 1, count), f32),
                pltpu.VMEM((width, 1, 128), f32),
                pltpu.VMEM((lines + total_lines, 1, 128), f32),
                pltpu.VMEM((n, lines, 1, 128), f32),
                pltpu.VMEM((group + 1, max(8, RAW), half), f32),
                dma((SPLIT + 1, held // min(load_rows(held)))),
                dma((1,)),
                dma((1,)),
                dma((SPLIT + 1,)),
                dma((2,)),
                dma((2,)),
                dma((SPLIT,)),
                dma((1,)),
                dma((1,)),
                dma((1,)),
                dma((1,)),
                dma((4,)),
                dma((4,)),
                dma((max(1, group - 1), 5)),
                dma((max(1, group - 1), 5)),
                dma((max(1, layers - 1), k_count - 2)),
                dma((n, 2)),
                dma((group + 1,)),
                dma((group + 1,)),
            ],
            compiler_params=pltpu.CompilerParams(
                collective_id=0, has_side_effects=True, vmem_limit_bytes=VMEM_LIMIT
            ),
            name="gather",
        )(*(pltpu.with_memory_space_constraint(a, pltpu.HBM) for a in arrays))
        gate, up, whole_gate, whole_up, scale_gate, scale_up, serve = pl.pallas_call(
            finish_kernel,
            out_shape=(
                jax.ShapeDtypeStruct((n, held, columns), bf16),
                jax.ShapeDtypeStruct((n, held, columns), bf16),
                jax.ShapeDtypeStruct((held, columns), f32),
                jax.ShapeDtypeStruct((held, columns), f32),
                jax.ShapeDtypeStruct((1, columns), f32),
                jax.ShapeDtypeStruct((1, columns), f32),
                jax.ShapeDtypeStruct((total_lines, 128), bf16),
            ),
            in_specs=[any_space] * 4,
            out_specs=(hbm_space,) * 7,
            scratch_shapes=[dma((7,))],
            compiler_params=pltpu.CompilerParams(vmem_limit_bytes=1 << 20),
            cost_estimate=pl.CostEstimate(flops=FLOPS, bytes_accessed=0, transcendentals=0),
            name="finish",
        )(*results[:4])
        if hidden:
            inner = [(group, 0), ((layers - 2) * group, (layers - 1) * group)]
            ring = [(a + i, b + i) for a, b in inner for i in range(group)]
            swap = [(i, i + 1 - 2 * (i % 2)) for i in range(n)]
            far = lax.ppermute(results[4], "shard", ring)
            near = lax.ppermute(results[5], "shard", swap)
            up = pl.pallas_call(
                functools.partial(patch_kernel, layers, group, stop - held),
                out_shape=jax.ShapeDtypeStruct((n, held, columns), bf16),
                in_specs=[any_space] * 3,
                out_specs=any_space,
                scratch_shapes=[dma((3,))],
                input_output_aliases={2: 0},
                compiler_params=pltpu.CompilerParams(vmem_limit_bytes=1 << 20),
                name="patch",
            )(far, near, up)
        return (
            gate.reshape(-1, columns), up.reshape(-1, columns), scale_gate.reshape(-1), scale_up.reshape(-1),
            serve.reshape(-1), whole_gate, whole_up,
        )

    return jax.shard_map(
        body,
        mesh=mesh,
        in_specs=(P("shard", "width"),) * 6 + (P(("shard", "width")),) * 2,
        out_specs=(
            P(None, "width"),
            P(None, "width"),
            P("width"),
            P("width"),
            P(),
            P("shard", "width"),
            P("shard", "width"),
        ),
        check_vma=False,
    )
```
